32 devices in a mesh: dp: 1 (over z), fsdp: 32 (over y, x, core).
Axes of the slice: x: 4, y: 4, z: 1, core: 2. Of those that a mesh axis runs over, the one named last changes fastest.
The devices are a block of a 4x4x8 slice.
Arguments:
- hidden: bfloat16 [32, 1024, 2048], P(('dp', 'fsdp'))
- g_attn: bfloat16 [2048], P('fsdp')
- w_query: bfloat16 [2048, 2048], P('fsdp')
- w_key: bfloat16 [2048, 512], P('fsdp')
- w_value: bfloat16 [2048, 512], P('fsdp')
- w_out: bfloat16 [2048, 2048], P('fsdp')
- g_mlp: bfloat16 [2048], P('fsdp')
- w_gate: bfloat16 [2048, 8192], P('fsdp')
- w_up: bfloat16 [2048, 8192], P('fsdp')
- w_down: bfloat16 [8192, 2048], P('fsdp')
- cos_tab: float32 [1024, 32], replicated
- sin_tab: float32 [1024, 32], replicated
Outputs:
- output 1: bfloat16 [32, 1024, 2048], P(('dp', 'fsdp'))
- output 2: bfloat16 [32, 1024, 8, 64], P(('dp', 'fsdp'))
- output 3: bfloat16 [32, 1024, 8, 64], P(('dp', 'fsdp'))
All inputs are finite; a program needn't handle non-finite values.
Results may differ from the reference program's by a relative error of at most 0.0190543.
Values are sent between devices in bfloat16 or wider.
A program may use at most 768 MiB of HBM per device.

```python
import jax
import jax.numpy as jnp
from jax import lax

BATCH_ROWS = 32
SEQ_LEN = 1024
MODEL_DIM = 2048
NUM_HEADS = 32
KV_HEADS = 8
HEAD_DIM = 64
FFN_DIM = 8192
QUERY_BLOCK = 256
ROPE_BASE = 500000.0
NORM_EPS = 1e-5


def make_weight(rng_key, fan_in, fan_out, factor):
    normal_draw = jax.random.normal(rng_key, (fan_in, fan_out), jnp.float32)
    return (normal_draw * (factor * fan_in ** -0.5)).astype(jnp.bfloat16)


def make_gain(rng_key):
    return jax.random.uniform(rng_key, (MODEL_DIM,), jnp.float32, 0.5, 1.5).astype(jnp.bfloat16)


def rope_tables(rng_key):
    start_pos = jax.random.randint(rng_key, (), 0, 8192)
    inv_freq = 1.0 / (ROPE_BASE ** (jnp.arange(0, HEAD_DIM, 2).astype(jnp.float32) / HEAD_DIM))
    positions = (start_pos + jnp.arange(SEQ_LEN)).astype(jnp.float32)
    angles = positions[:, None] * inv_freq[None, :]
    return jnp.cos(angles), jnp.sin(angles)


def setup_inputs(seed: int = 0, part: int = 0) -> dict:
    sub_keys = jax.random.split(jax.random.key(seed), 11)
    part_key = jax.random.fold_in(sub_keys[0], part)
    q_width = NUM_HEADS * HEAD_DIM
    kv_width = KV_HEADS * HEAD_DIM
    hidden = 0.5 * jax.random.normal(part_key, (BATCH_ROWS, SEQ_LEN, MODEL_DIM), jnp.float32)
    cos_tab, sin_tab = rope_tables(sub_keys[10])
    return {
        "hidden": hidden.astype(jnp.bfloat16),
        "g_attn": make_gain(sub_keys[1]),
        "w_query": make_weight(sub_keys[2], MODEL_DIM, q_width, 2.0),
        "w_key": make_weight(sub_keys[3], MODEL_DIM, kv_width, 1.0),
        "w_value": make_weight(sub_keys[4], MODEL_DIM, kv_width, 1.0),
        "w_out": make_weight(sub_keys[5], q_width, MODEL_DIM, 1.0),
        "g_mlp": make_gain(sub_keys[6]),
        "w_gate": make_weight(sub_keys[7], MODEL_DIM, FFN_DIM, 1.0),
        "w_up": make_weight(sub_keys[8], MODEL_DIM, FFN_DIM, 1.0),
        "w_down": make_weight(sub_keys[9], FFN_DIM, MODEL_DIM, 1.0),
        "cos_tab": cos_tab,
        "sin_tab": sin_tab,
    }


def rms_norm(rows_in, gain_vec):
    upcast = rows_in.astype(jnp.float32)
    scaled = upcast * lax.rsqrt(jnp.mean(upcast * upcast, axis=-1, keepdims=True) + NORM_EPS)
    return (scaled * gain_vec.astype(jnp.float32)).astype(jnp.bfloat16)


def apply_rope(heads_in, cos_tab, sin_tab):
    half_dim = HEAD_DIM // 2
    upcast = heads_in.astype(jnp.float32)
    lo_half = upcast[..., :half_dim]
    hi_half = upcast[..., half_dim:]
    cos_bc = cos_tab[:, None, :]
    sin_bc = sin_tab[:, None, :]
    rotated = jnp.concatenate([lo_half * cos_bc - hi_half * sin_bc, hi_half * cos_bc + lo_half * sin_bc], axis=-1)
    return rotated.astype(jnp.bfloat16)


def reference(hidden, g_attn, w_query, w_key, w_value, w_out, g_mlp, w_gate, w_up, w_down, cos_tab, sin_tab):
    group_size = NUM_HEADS // KV_HEADS
    key_pos = jnp.arange(SEQ_LEN)

    def one_sequence(seq_in):
        normed = rms_norm(seq_in, g_attn)
        query_proj = jnp.dot(normed, w_query, preferred_element_type=jnp.float32).astype(jnp.bfloat16)
        key_proj = jnp.dot(normed, w_key, preferred_element_type=jnp.float32).astype(jnp.bfloat16)
        value_proj = jnp.dot(normed, w_value, preferred_element_type=jnp.float32).astype(jnp.bfloat16)
        query_rot = apply_rope(query_proj.reshape(SEQ_LEN, NUM_HEADS, HEAD_DIM), cos_tab, sin_tab)
        key_rot = apply_rope(key_proj.reshape(SEQ_LEN, KV_HEADS, HEAD_DIM), cos_tab, sin_tab)
        value_heads = value_proj.reshape(SEQ_LEN, KV_HEADS, HEAD_DIM)
        query_grp = query_rot.reshape(SEQ_LEN, KV_HEADS, group_size, HEAD_DIM).astype(jnp.float32)
        key_wide = key_rot.astype(jnp.float32)
        value_wide = value_heads.astype(jnp.float32)

        def one_block(block_idx):
            blk_start = block_idx * QUERY_BLOCK
            query_blk = lax.dynamic_slice_in_dim(query_grp, blk_start, QUERY_BLOCK, axis=0)
            scores = jnp.einsum("qkgd,skd->kgqs", query_blk, key_wide) * HEAD_DIM ** -0.5
            query_pos = blk_start + jnp.arange(QUERY_BLOCK)
            scores = jnp.where(key_pos[None, :] <= query_pos[:, None], scores, -jnp.inf)
            prob_bf16 = jax.nn.softmax(scores, axis=-1).astype(jnp.bfloat16)
            mixed_vals = jnp.einsum("kgqs,skd->qkgd", prob_bf16.astype(jnp.float32), value_wide)
            return mixed_vals.astype(jnp.bfloat16)

        attn_heads = lax.map(one_block, jnp.arange(SEQ_LEN // QUERY_BLOCK))
        attn_flat = attn_heads.reshape(SEQ_LEN, NUM_HEADS * HEAD_DIM)
        attn_proj = jnp.dot(attn_flat, w_out, preferred_element_type=jnp.float32).astype(jnp.bfloat16)
        residual = (seq_in.astype(jnp.float32) + attn_proj.astype(jnp.float32)).astype(jnp.bfloat16)
        normed_mlp = rms_norm(residual, g_mlp)
        gate_proj = jnp.dot(normed_mlp, w_gate, preferred_element_type=jnp.float32).astype(jnp.bfloat16)
        up_proj = jnp.dot(normed_mlp, w_up, preferred_element_type=jnp.float32).astype(jnp.bfloat16)
        act_in = (jax.nn.silu(gate_proj.astype(jnp.float32)) * up_proj.astype(jnp.float32)).astype(jnp.bfloat16)
        mlp_out = jnp.dot(act_in, w_down, preferred_element_type=jnp.float32).astype(jnp.bfloat16)
        out_seq = (residual.astype(jnp.float32) + mlp_out.astype(jnp.float32)).astype(jnp.bfloat16)
        return out_seq, key_rot, value_heads

    out_hidden, k_cache, v_cache = lax.map(one_sequence, hidden)
    return (out_hidden, k_cache, v_cache)
```

```python
import functools
import math
import jax
import jax.numpy as jnp
from jax import lax
from jax.experimental import pallas as pl
from jax.experimental.pallas import tpu as pltpu
from jax.sharding import PartitionSpec as P

NORM_EPS = 1e-5
MESH = pl.DeviceIdType.MESH
LAG = 1
SLOTS = 2 * LAG + 2
READY = 4 * LAG + 1
ATTN_TICKS = (1, 2, 4, 4)
ROW_BLOCK = 256
BF16 = jnp.bfloat16
F32 = jnp.float32


def layer_kernel(cfg, x_hbm, gain_hbm, wq, wk, wv, wo, wg, wu, wd, cos_hbm, sin_hbm,
                 out_hbm, kt_hbm, vt_hbm, gath, gath_d, gath_g,
                 xv, hbuf, qbuf, rbuf, wbuf, wbuf_d, wl, wl_d, wl_g, gvm, gains, cosv, sinv,
                 send_sem, recv_sem, own_sem, load_sem, wsem, misc_sem, out_sem):
    side, seq, dim, ffn = cfg["side"], cfg["seq"], cfg["dim"], cfg["ffn"]
    width, half_w, width_d = cfg["width"], cfg["width"] // 2, cfg["width_d"]
    kv_dim = cfg["kv_dim"]
    n_q, n_o = cfg["q_dim"] // width, dim // width
    n_ffn, n_down = ffn // half_w, dim // width_d
    first_o = 1 + n_q
    first_f = first_o + n_o
    first_d = first_f + n_ffn
    n_piece = first_d + n_down
    rows, rows_d = cfg["rows"], cfg["rows_d"]
    rb = min(ROW_BLOCK, seq)

    me = lax.axis_index("fsdp")
    core = lax.rem(me, 2)
    px = lax.rem(me // 2, side)
    py = me // (2 * side)
    pa = px + core * (py - px)
    pb = py + core * (px - py)
    a_up, a_dn = lax.rem(pa + 1, side), lax.rem(pa + side - 1, side)
    b_up, b_dn = lax.rem(pb + 1, side), lax.rem(pb + side - 1, side)

    def device_at(a, b):
        y = b + core * (a - b)
        x = a + core * (b - a)
        return (y * side + x) * 2 + core

    dev_ap, dev_am = device_at(a_up, pb), device_at(a_dn, pb)
    dev_bp, dev_bm = device_at(pa, b_up), device_at(pa, b_dn)
    sibling = me + 1 - 2 * core

    def load(src, dst, sem):
        pltpu.make_async_copy(src, dst, sem).start()

    load(gain_hbm, wl_g, load_sem.at[n_piece])
    load(wk, wl.at[0, :, pl.ds(0, kv_dim)], load_sem.at[0])
    load(wv, wl.at[0, :, pl.ds(kv_dim, kv_dim)], load_sem.at[0])
    for c in range(n_q):
        load(wq.at[:, pl.ds(c * width, width)], wl.at[1 + c], load_sem.at[1 + c])
    load(x_hbm, xv, misc_sem.at[0])
    load(cos_hbm, cosv, misc_sem.at[1])
    load(sin_hbm, sinv, misc_sem.at[2])
    for c in range(n_o):
        load(wo.at[:, pl.ds(c * width, width)], wl.at[first_o + c], load_sem.at[first_o + c])

    def load_ffn(j, carry):
        col = pl.multiple_of(j * half_w, half_w)
        load(wg.at[:, pl.ds(col, half_w)], wl.at[first_f + j, :, pl.ds(0, half_w)], load_sem.at[first_f + j])
        load(wu.at[:, pl.ds(col, half_w)], wl.at[first_f + j, :, pl.ds(half_w, half_w)], load_sem.at[first_f + j])
        return carry

    lax.fori_loop(0, n_ffn, load_ffn, 0)

    def load_down(j, carry):
        col = pl.multiple_of(j * width_d, width_d)
        load(wd.at[:, pl.ds(col, width_d)], wl_d.at[j], load_sem.at[first_d + j])
        return carry

    lax.fori_loop(0, n_down, load_down, 0)

    dp = lax.axis_index("dp")
    barrier = pltpu.get_barrier_semaphore()
    for peer in (dev_ap, dev_am, dev_bp, dev_bm, sibling):
        pl.semaphore_signal(barrier, inc=1, device_id=(dp, peer), device_id_type=MESH)
    pl.semaphore_wait(barrier, 5)

    def remote(src, dst, stage, way, slot, peer):
        return pltpu.make_async_remote_copy(
            src_ref=src, dst_ref=dst, send_sem=send_sem.at[stage, way, slot], recv_sem=recv_sem.at[stage, way, slot],
            device_id=(dp, peer), device_id_type=MESH)

    def stage_op(stage, own, buf, n_rows, slot, wait_own):
        h = n_rows // 2
        mine = buf.at[core, pb, pa]

        def s1():
            return (remote(own, mine, 0, 0, slot, dev_ap), remote(own, mine, 0, 1, slot, dev_am))

        def s1_in():
            lo, hi = buf.at[core, pb, a_dn], buf.at[core, pb, a_up]
            return (remote(lo, lo, 0, 0, slot, dev_ap), remote(hi, hi, 0, 1, slot, dev_am))

        def s2():
            lo, hi = buf.at[core, pb, a_dn, pl.ds(0, h)], buf.at[core, pb, a_up, pl.ds(h, h)]
            return (remote(lo, lo, 1, 0, slot, dev_ap), remote(hi, hi, 1, 1, slot, dev_am))

        def s2_in():
            far = lax.rem(pa + 2, side)
            lo, hi = buf.at[core, pb, far, pl.ds(0, h)], buf.at[core, pb, far, pl.ds(h, h)]
            return (remote(lo, lo, 1, 0, slot, dev_ap), remote(hi, hi, 1, 1, slot, dev_am))

        def s3():
            line = buf.at[core, pb]
            return (remote(line, line, 2, 0, slot, dev_bp), remote(line, line, 2, 1, slot, dev_bm))

        def s3_in():
            lo, hi = buf.at[core, b_dn], buf.at[core, b_up]
            return (remote(lo, lo, 2, 0, slot, dev_bp), remote(hi, hi, 2, 1, slot, dev_bm))

        def s4():
            lo, hi = buf.at[core, b_dn, pl.ds(0, side // 2)], buf.at[core, b_up, pl.ds(side // 2, side // 2)]
            return (remote(lo, lo, 3, 0, slot, dev_bp), remote(hi, hi, 3, 1, slot, dev_bm))

        def s4_in():
            far = lax.rem(pb + 2, side)
            lo, hi = buf.at[core, far, pl.ds(0, side // 2)], buf.at[core, far, pl.ds(side // 2, side // 2)]
            return (remote(lo, lo, 3, 0, slot, dev_bp), remote(hi, hi, 3, 1, slot, dev_bm))

        def s5():
            plane = buf.at[core]
            return (remote(plane, plane, 4, 0, slot, sibling),)

        def s5_in():
            plane = buf.at[1 - core]
            return (remote(plane, plane, 4, 0, slot, sibling),)

        outs = (s1, s2, s3, s4, s5)
        ins = (s1_in, s2_in, s3_in, s4_in, s5_in)

        def keep():
            return pltpu.make_async_copy(own, mine, own_sem.at[slot])

        if stage == 0:
            wait_own()
            keep().start()
        else:
            for d in outs[stage - 1]():
                d.wait_send()
            for d in ins[stage - 1]():
                d.wait_recv()
            if stage == 2:
                keep().wait()
        if stage < 5:
            for d in outs[stage]():
                d.start()

    def run_stage(stage, p):
        slot = lax.rem(p, SLOTS)

        @pl.when(p == 0)
        def _():
            stage_op(stage, wl_g, gath_g, wl_g.shape[0], SLOTS,
                     lambda: pltpu.make_async_copy(wl_g, wl_g, load_sem.at[n_piece]).wait())

        @pl.when(jnp.logical_and(p >= 0, p < first_d))
        def _():
            own = wl.at[p]
            stage_op(stage, own, gath.at[p], rows, slot,
                     lambda: pltpu.make_async_copy(own, own, load_sem.at[p]).wait())

        @pl.when(jnp.logical_and(p >= first_d, p < n_piece))
        def _():
            own = wl_d.at[p - first_d]
            stage_op(stage, own, gath_d.at[p - first_d], rows_d, slot,
                     lambda: pltpu.make_async_copy(own, own, load_sem.at[p]).wait())

    def tick(t):
        for stage in range(5):
            run_stage(stage, t - stage * LAG)
        run_stage(5, t - READY)

    def fetch(buf, dst, sem):
        cps = [pltpu.make_async_copy(buf.at[0], dst.at[:, :, 0], sem)]
        for y in range(side):
            cps.append(pltpu.make_async_copy(buf.at[1, :, y], dst.at[y, :, 1], sem))
        for cp in cps:
            cp.start()

    def fetch_piece(p):
        slot = lax.rem(p, 2)
        fetch(gath.at[p], wbuf.at[slot], wsem.at[slot])

    def wait_piece(p):
        slot = lax.rem(p, 2)
        pltpu.make_async_copy(wbuf.at[slot], wbuf.at[slot], wsem.at[slot]).wait()
        return slot

    def fetch_down(i):
        slot = lax.rem(i, 2)
        fetch(gath_d.at[i], wbuf_d.at[slot], wsem.at[2 + slot])

    def wait_down(i):
        slot = lax.rem(i, 2)
        pltpu.make_async_copy(wbuf_d.at[slot], wbuf_d.at[slot], wsem.at[2 + slot]).wait()
        return slot

    def row_loop(body, block=rb):
        def step(i, carry):
            body(pl.ds(pl.multiple_of(i * block, block), block))
            return carry

        lax.fori_loop(0, seq // block, step, 0)

    def norm_rows(src, dst, gain_row):
        nb = min(64, seq)

        def body(rs):
            xx = src[rs, :].astype(F32)
            scale = lax.rsqrt(jnp.mean(xx * xx, axis=-1, keepdims=True) + NORM_EPS)
            dst[rs, :] = ((xx * scale) * gains[pl.ds(gain_row, 1), :]).astype(BF16)

        row_loop(body, nb)

    def weight(slot):
        return wbuf[slot].reshape(dim, width)

    lane = lax.broadcasted_iota(jnp.int32, (rb, 128), 1)
    low_half = lax.rem(lane, cfg["head"]) < cfg["head"] // 2

    def rope(block, rs):
        up = block.astype(BF16).astype(F32)
        swapped = jnp.where(low_half, pltpu.roll(up, 128 - cfg["head"] // 2, 1), pltpu.roll(up, cfg["head"] // 2, 1))
        return up * cosv[rs, :] + swapped * sinv[rs, :]

    n_kv = kv_dim // cfg["head"]
    head = cfg["head"]
    col_v = (0, n_kv * 128)
    col_k = (2 * n_kv * 128, 2 * n_kv * 128 + seq)
    col_t = 2 * n_kv * 128 + 2 * seq

    def pre(t, carry):
        tick(t)
        return carry

    lax.fori_loop(0, READY + 1, pre, 0)
    fetch_piece(0)
    pltpu.sync_copy(gath_g, gvm)
    pltpu.make_async_copy(x_hbm, xv, misc_sem.at[0]).wait()
    pltpu.make_async_copy(cos_hbm, cosv, misc_sem.at[1]).wait()
    pltpu.make_async_copy(sin_hbm, sinv, misc_sem.at[2]).wait()
    lane8 = lax.broadcasted_iota(jnp.int32, (8, 128), 1)
    for y in range(side):
        for x in range(side):
            for which in range(2):
                even = gvm[0, y, x, 8 * which:8 * which + 8, :]
                odd = gvm[1, x, y, 8 * which:8 * which + 8, :]
                c = (y * side + x) * 128
                gains[8 * which:8 * which + 8, c:c + 128] = jnp.where(lane8 < 64, even, odd)
    norm_rows(xv, hbuf, 0)

    tick(READY + 1)
    fetch_piece(1)
    slot = wait_piece(0)

    def kv_block(rs):
        acc = jnp.dot(hbuf[rs, :], weight(slot), preferred_element_type=F32)
        first = lane < head
        for c in range(kv_dim // 128):
            kr = rope(acc[:, c * 128:(c + 1) * 128], rs)
            kt = jnp.transpose(kr).astype(BF16)
            rbuf[c * 128:(c + 1) * 128, pl.ds(col_t + rs.start, rs.size)] = kt
            zero = jnp.zeros((head, rs.size), BF16)
            for g in range(2):
                kk = kt[g * head:(g + 1) * head]
                r0 = (2 * c + g) * 128
                rbuf[r0:r0 + head, pl.ds(col_k[0] + rs.start, rs.size)] = kk
                rbuf[r0 + head:r0 + 128, pl.ds(col_k[0] + rs.start, rs.size)] = zero
                rbuf[r0:r0 + head, pl.ds(col_k[1] + rs.start, rs.size)] = zero
                rbuf[r0 + head:r0 + 128, pl.ds(col_k[1] + rs.start, rs.size)] = kk
            vv = acc[:, kv_dim + c * 128:kv_dim + (c + 1) * 128]
            vt = jnp.transpose(vv).astype(BF16)
            rbuf[kv_dim + c * 128:kv_dim + (c + 1) * 128, pl.ds(col_t + rs.start, rs.size)] = vt
            turned = pltpu.roll(vv, head, 1)
            g0, g1 = 2 * c, 2 * c + 1
            rbuf[rs, col_v[0] + g0 * 128:col_v[0] + g0 * 128 + 128] = jnp.where(first, vv, 0.0).astype(BF16)
            rbuf[rs, col_v[1] + g0 * 128:col_v[1] + g0 * 128 + 128] = jnp.where(first, 0.0, turned).astype(BF16)
            rbuf[rs, col_v[0] + g1 * 128:col_v[0] + g1 * 128 + 128] = jnp.where(first, turned, 0.0).astype(BF16)
            rbuf[rs, col_v[1] + g1 * 128:col_v[1] + g1 * 128 + 128] = jnp.where(first, 0.0, vv).astype(BF16)

    row_loop(kv_block)
    kt_out = pltpu.make_async_copy(rbuf.at[pl.ds(0, kv_dim), pl.ds(col_t, seq)], kt_hbm, out_sem.at[n_down])
    vt_out = pltpu.make_async_copy(rbuf.at[pl.ds(kv_dim, kv_dim), pl.ds(col_t, seq)], vt_hbm, out_sem.at[n_down + 1])
    kt_out.start()
    vt_out.start()

    def q_step(c, carry):
        tick(READY + 2 + c)
        fetch_piece(2 + c)
        slot = wait_piece(1 + c)

        def q_block(rs):
            acc = jnp.dot(hbuf[rs, :], weight(slot), preferred_element_type=F32)
            for k in range(width // 128):
                dst = pl.ds(pl.multiple_of(c * width + k * 128, 128), 128)
                qbuf[rs, dst] = rope(acc[:, k * 128:(k + 1) * 128], rs).astype(BF16)

        row_loop(q_block)
        return carry

    lax.fori_loop(0, n_q, q_step, 0)
    t_now = READY + 2 + n_q

    n_pair = cfg["q_dim"] // 128
    pairs_per_kv = n_pair // n_kv
    qb = seq // len(ATTN_TICKS)
    scale = math.log2(math.e) * head ** -0.5
    causal = lax.broadcasted_iota(jnp.int32, (qb, qb), 0) >= lax.broadcasted_iota(jnp.int32, (qb, qb), 1)
    for i, n_t in enumerate(ATTN_TICKS):
        past = i * qb
        per = n_pair // n_t

        def one_pair(pi, i=i, past=past):
            g = pi // pairs_per_kv
            cs = pl.ds(pl.multiple_of(pi * 128, 128), 128)
            qp = qbuf[i * qb:(i + 1) * qb, cs]
            krow = pl.ds(pl.multiple_of(g * 128, 128), 128)
            total = None
            for hf in range(2):
                s_d = jnp.dot(qp, rbuf[krow, col_k[hf] + past:col_k[hf] + past + qb], preferred_element_type=F32)
                s_d = jnp.where(causal, s_d, -jnp.inf)
                m = jnp.max(s_d, axis=-1, keepdims=True)
                if past:
                    s_p = jnp.dot(qp, rbuf[krow, col_k[hf]:col_k[hf] + past], preferred_element_type=F32)
                    m = jnp.maximum(m, jnp.max(s_p, axis=-1, keepdims=True))
                e_d = jnp.exp2((s_d - m) * scale)
                den = jnp.sum(e_d, axis=-1, keepdims=True)
                if past:
                    e_p = jnp.exp2((s_p - m) * scale)
                    den = den + jnp.sum(e_p, axis=-1, keepdims=True)
                inv = 1.0 / den
                vcol = pl.ds(pl.multiple_of(col_v[hf] + g * 128, 128), 128)
                o = jnp.dot((e_d * inv).astype(BF16), rbuf[past:past + qb, vcol], preferred_element_type=F32)
                if past:
                    o = o + jnp.dot((e_p * inv).astype(BF16), rbuf[0:past, vcol], preferred_element_type=F32)
                total = o if total is None else total + o
            hbuf[i * qb:(i + 1) * qb, cs] = total.astype(BF16)

        def att_step(k, carry, one_pair=one_pair, per=per, base=t_now):
            tick(base + k)

            def inner(j, c2):
                one_pair(k * per + j)
                return c2

            lax.fori_loop(0, per, inner, 0)
            return carry

        lax.fori_loop(0, n_t, att_step, 0)
        t_now += n_t

    def o_step(c, carry):
        tick(t_now + c)
        fetch_piece(first_o + 1 + c)
        slot = wait_piece(first_o + c)

        def o_block(rs):
            acc = jnp.dot(hbuf[rs, :], weight(slot), preferred_element_type=F32)
            cs = pl.ds(pl.multiple_of(c * width, width), width)
            xv[rs, cs] = (xv[rs, cs].astype(F32) + acc.astype(BF16).astype(F32)).astype(BF16)

        row_loop(o_block)
        return carry

    lax.fori_loop(0, n_o, o_step, 0)
    t_now += n_o
    kt_out.wait()
    vt_out.wait()
    norm_rows(xv, qbuf, 8)

    def f_step(j, carry):
        @pl.when(lax.rem(j, 2) == 0)
        def _():
            tick(t_now + j // 2)

        @pl.when(j + 1 < n_ffn)
        def _():
            fetch_piece(first_f + j + 1)

        @pl.when(j + 1 == n_ffn)
        def _():
            fetch_down(0)

        slot = wait_piece(first_f + j)

        def f_block(rs):
            acc = jnp.dot(qbuf[rs, :], weight(slot), preferred_element_type=F32)
            gate = acc[:, :half_w].astype(BF16).astype(F32)
            up = acc[:, half_w:].astype(BF16).astype(F32)
            cs = pl.ds(pl.multiple_of(j * half_w, half_w), half_w)
            rbuf[rs, cs] = (jax.nn.silu(gate) * up).astype(BF16)

        row_loop(f_block)
        return carry

    lax.fori_loop(0, n_ffn, f_step, 0)
    t_now += (n_ffn + 1) // 2

    t_left = n_piece + READY - t_now
    skip = n_down - 1 - t_left

    def out_copy(i):
        cs = pl.ds(pl.multiple_of(i * width_d, width_d), width_d)
        return pltpu.make_async_copy(xv.at[:, cs], out_hbm.at[:, cs], out_sem.at[i])

    def d_step(i, carry):
        @pl.when(jnp.logical_and(i >= skip, i < n_down - 1))
        def _():
            tick(t_now + i - skip)

        @pl.when(i + 1 < n_down)
        def _():
            fetch_down(i + 1)

        slot = wait_down(i)
        cs = pl.ds(pl.multiple_of(i * width_d, width_d), width_d)

        def d_block(rs):
            acc = jnp.dot(rbuf[rs, :], wbuf_d[slot].reshape(ffn, width_d), preferred_element_type=F32)
            xv[rs, cs] = (xv[rs, cs].astype(F32) + acc.astype(BF16).astype(F32)).astype(BF16)

        row_loop(d_block)
        out_copy(i).start()
        return carry

    lax.fori_loop(0, n_down, d_step, 0)

    def finish(i, carry):
        out_copy(i).wait()
        return carry

    lax.fori_loop(0, n_down, finish, 0)
    assert skip >= 0 and sum(ATTN_TICKS) - skip <= n_down


def solution(mesh, width=1024, width_d=256):
    n_dev = mesh.shape["fsdp"]
    side = math.isqrt(n_dev // 2)
    tok_spec = P(("dp", "fsdp"), None, None)
    cache_spec = P(("dp", "fsdp"), None, None, None)
    row_spec = P("fsdp", None)
    gain_spec = P("fsdp")
    table_spec = P(None, None)

    def local_layer(hidden, g_attn, w_query, w_key, w_value, w_out, g_mlp, w_gate, w_up, w_down, cos_tab, sin_tab):
        _, seq, dim = hidden.shape
        rows, q_dim = w_query.shape
        kv_dim = w_key.shape[1]
        ffn = w_gate.shape[1]
        rows_d = w_down.shape[0]
        head = 2 * cos_tab.shape[1]
        cfg = dict(side=side, seq=seq, dim=dim, ffn=ffn, width=width, width_d=width_d, kv_dim=kv_dim, q_dim=q_dim,
                   rows=rows, rows_d=rows_d, head=head)
        assert 2 * kv_dim == width and rows == 64 and rows * n_dev == dim
        gain_tile = jnp.concatenate([
            jnp.broadcast_to(jnp.tile(g_attn.astype(F32), 2)[None, :], (8, 128)),
            jnp.broadcast_to(jnp.tile(g_mlp.astype(F32), 2)[None, :], (8, 128))], axis=0)
        cos4 = jnp.concatenate([cos_tab] * 4, axis=1)
        sin4 = jnp.concatenate([-sin_tab, sin_tab] * 2, axis=1)
        n_wide = (2 * kv_dim + q_dim + dim + 2 * ffn) // width
        n_down = dim // width_d
        n_piece = n_wide + n_down
        hbm = pl.BlockSpec(memory_space=pl.ANY)
        res = pl.pallas_call(
            functools.partial(layer_kernel, cfg),
            out_shape=(
                jax.ShapeDtypeStruct((seq, dim), BF16),
                jax.ShapeDtypeStruct((kv_dim, seq), BF16),
                jax.ShapeDtypeStruct((kv_dim, seq), BF16),
                jax.ShapeDtypeStruct((n_wide, 2, side, side, rows, width), BF16),
                jax.ShapeDtypeStruct((n_down, 2, side, side, rows_d, width_d), BF16),
                jax.ShapeDtypeStruct((2, side, side, 16, 128), F32)),
            in_specs=[hbm] * 11,
            out_specs=[hbm] * 6,
            scratch_shapes=[
                pltpu.VMEM((seq, dim), BF16),
                pltpu.VMEM((seq, max(dim, q_dim)), BF16),
                pltpu.VMEM((seq, max(dim, q_dim)), BF16),
                pltpu.VMEM((max(seq, 2 * kv_dim), ffn), BF16),
                pltpu.VMEM((2, side, side, 2, rows, width), BF16),
                pltpu.VMEM((2, side, side, 2, rows_d, width_d), BF16),
                pltpu.VMEM((n_wide, rows, width), BF16),
                pltpu.VMEM((n_down, rows_d, width_d), BF16),
                pltpu.VMEM((16, 128), F32),
                pltpu.VMEM((2, side, side, 16, 128), F32),
                pltpu.VMEM((16, dim), F32),
                pltpu.VMEM((seq, 128), F32),
                pltpu.VMEM((seq, 128), F32),
                pltpu.SemaphoreType.DMA((5, 2, SLOTS + 1)),
                pltpu.SemaphoreType.DMA((5, 2, SLOTS + 1)),
                pltpu.SemaphoreType.DMA((SLOTS + 1,)),
                pltpu.SemaphoreType.DMA((n_piece + 1,)),
                pltpu.SemaphoreType.DMA((4,)),
                pltpu.SemaphoreType.DMA((3,)),
                pltpu.SemaphoreType.DMA((n_down + 2,)),
            ],
            compiler_params=pltpu.CompilerParams(
                collective_id=0, has_side_effects=True, vmem_limit_bytes=67043328),
        )(hidden[0], gain_tile, w_query, w_key, w_value, w_out, w_gate, w_up, w_down, cos4, sin4)
        out, kt, vt = res[:3]

        def cache(t):
            return jnp.transpose(t.reshape(1, kv_dim // head, head, seq), (0, 3, 1, 2))

        return out[None], cache(kt), cache(vt)

    return jax.shard_map(local_layer, mesh=mesh, in_specs=(tok_spec, gain_spec, row_spec, row_spec, row_spec, row_spec, gain_spec, row_spec, row_spec, row_spec, table_spec, table_spec), out_specs=(tok_spec, cache_spec, cache_spec), check_vma=False)
```

```python
import functools
import math
import jax
import jax.numpy as jnp
from jax import lax
from jax.experimental import pallas as pl
from jax.experimental.pallas import tpu as pltpu
from jax.sharding import PartitionSpec as P

NORM_EPS = 1e-5
MESH = pl.DeviceIdType.MESH
LAG = 2
SLOTS = 2 * LAG + 4
READY = 4 * LAG + 1
ATTN_TICKS = (1, 2, 4, 4)
ROW_BLOCK = 256
BF16 = jnp.bfloat16
F32 = jnp.float32


def layer_kernel(cfg, x_hbm, gain_hbm, wq, wk, wv, wo, wg, wu, wd, cos_hbm, sin_hbm,
                 out_hbm, kt_hbm, vt_hbm, gath, gath_d, gath_g,
                 xv, hbuf, qbuf, rbuf, wbuf, wbuf_d, wl, wl_d, wl_g, gvm, gains, cosv, sinv, cost, sint,
                 send_sem, recv_sem, own_sem, load_sem, wsem, misc_sem, out_sem):
    side, seq, dim, ffn = cfg["side"], cfg["seq"], cfg["dim"], cfg["ffn"]
    width, half_w, width_d = cfg["width"], cfg["width"] // 2, cfg["width_d"]
    kv_dim = cfg["kv_dim"]
    n_q, n_o = cfg["q_dim"] // width, dim // width
    n_ffn, n_down = ffn // half_w, dim // width_d
    first_o = 1 + n_q
    first_f = first_o + n_o
    first_d = first_f + n_ffn
    n_piece = first_d + n_down
    rows, rows_d = cfg["rows"], cfg["rows_d"]
    rb = min(ROW_BLOCK, seq)
    tb = min(128, seq)

    me = lax.axis_index("fsdp")
    core = lax.rem(me, 2)
    px = lax.rem(me // 2, side)
    py = me // (2 * side)
    pa = px + core * (py - px)
    pb = py + core * (px - py)
    a_up, a_dn = lax.rem(pa + 1, side), lax.rem(pa + side - 1, side)
    b_up, b_dn = lax.rem(pb + 1, side), lax.rem(pb + side - 1, side)

    def device_at(a, b):
        y = b + core * (a - b)
        x = a + core * (b - a)
        return (y * side + x) * 2 + core

    dev_ap, dev_am = device_at(a_up, pb), device_at(a_dn, pb)
    dev_bp, dev_bm = device_at(pa, b_up), device_at(pa, b_dn)
    sibling = me + 1 - 2 * core

    def load(src, dst, sem):
        pltpu.make_async_copy(src, dst, sem).start()

    load(gain_hbm, wl_g, load_sem.at[n_piece])
    load(wk, wl.at[0, :, pl.ds(0, kv_dim)], load_sem.at[0])
    load(wv, wl.at[0, :, pl.ds(kv_dim, kv_dim)], load_sem.at[0])
    for c in range(n_q):
        load(wq.at[:, pl.ds(c * width, width)], wl.at[1 + c], load_sem.at[1 + c])
    load(x_hbm, xv, misc_sem.at[0])
    load(cos_hbm, cost, misc_sem.at[1])
    load(sin_hbm, sint, misc_sem.at[2])
    for c in range(n_o):
        load(wo.at[:, pl.ds(c * width, width)], wl.at[first_o + c], load_sem.at[first_o + c])

    def load_ffn(j, carry):
        col = pl.multiple_of(j * half_w, half_w)
        load(wg.at[:, pl.ds(col, half_w)], wl.at[first_f + j, :, pl.ds(0, half_w)], load_sem.at[first_f + j])
        load(wu.at[:, pl.ds(col, half_w)], wl.at[first_f + j, :, pl.ds(half_w, half_w)], load_sem.at[first_f + j])
        return carry

    lax.fori_loop(0, n_ffn, load_ffn, 0)

    def load_down(j, carry):
        col = pl.multiple_of(j * width_d, width_d)
        load(wd.at[:, pl.ds(col, width_d)], wl_d.at[j], load_sem.at[first_d + j])
        return carry

    lax.fori_loop(0, n_down, load_down, 0)

    dp = lax.axis_index("dp")
    barrier = pltpu.get_barrier_semaphore()
    for peer in (dev_ap, dev_am, dev_bp, dev_bm, sibling):
        pl.semaphore_signal(barrier, inc=1, device_id=(dp, peer), device_id_type=MESH)
    pl.semaphore_wait(barrier, 5)

    def remote(src, dst, stage, way, slot, peer):
        return pltpu.make_async_remote_copy(
            src_ref=src, dst_ref=dst, send_sem=send_sem.at[stage, way, slot], recv_sem=recv_sem.at[stage, way, slot],
            device_id=(dp, peer), device_id_type=MESH)

    def stage_op(stage, own, buf, n_rows, slot, wait_own):
        h = n_rows // 2
        mine = buf.at[core, pb, pa]

        def s1():
            return (remote(own, mine, 0, 0, slot, dev_ap), remote(own, mine, 0, 1, slot, dev_am))

        def s1_in():
            lo, hi = buf.at[core, pb, a_dn], buf.at[core, pb, a_up]
            return (remote(lo, lo, 0, 0, slot, dev_ap), remote(hi, hi, 0, 1, slot, dev_am))

        def s2():
            lo, hi = buf.at[core, pb, a_dn, pl.ds(0, h)], buf.at[core, pb, a_up, pl.ds(h, h)]
            return (remote(lo, lo, 1, 0, slot, dev_ap), remote(hi, hi, 1, 1, slot, dev_am))

        def s2_in():
            far = lax.rem(pa + 2, side)
            lo, hi = buf.at[core, pb, far, pl.ds(0, h)], buf.at[core, pb, far, pl.ds(h, h)]
            return (remote(lo, lo, 1, 0, slot, dev_ap), remote(hi, hi, 1, 1, slot, dev_am))

        def s3():
            line = buf.at[core, pb]
            return (remote(line, line, 2, 0, slot, dev_bp), remote(line, line, 2, 1, slot, dev_bm))

        def s3_in():
            lo, hi = buf.at[core, b_dn], buf.at[core, b_up]
            return (remote(lo, lo, 2, 0, slot, dev_bp), remote(hi, hi, 2, 1, slot, dev_bm))

        def s4():
            lo, hi = buf.at[core, b_dn, pl.ds(0, side // 2)], buf.at[core, b_up, pl.ds(side // 2, side // 2)]
            return (remote(lo, lo, 3, 0, slot, dev_bp), remote(hi, hi, 3, 1, slot, dev_bm))

        def s4_in():
            far = lax.rem(pb + 2, side)
            lo, hi = buf.at[core, far, pl.ds(0, side // 2)], buf.at[core, far, pl.ds(side // 2, side // 2)]
            return (remote(lo, lo, 3, 0, slot, dev_bp), remote(hi, hi, 3, 1, slot, dev_bm))

        def hand(line, row, way):
            ref = buf.at[core, line]
            return remote(ref, ref, row, way, slot, sibling)

        def hand_in(line, row, way):
            ref = buf.at[1 - core, line]
            return remote(ref, ref, row, way, slot, sibling)

        def s3_all():
            return s3() + (hand(pb, 4, 0),)

        def s4_all():
            return s4() + (hand(b_dn, 4, 1), hand(b_up, 5, 0))

        def s5():
            return (hand(lax.rem(pb + 2, side), 5, 1),)

        def s5_in():
            return (hand_in(pa, 4, 0), hand_in(a_dn, 4, 1), hand_in(a_up, 5, 0), hand_in(lax.rem(pa + 2, side), 5, 1))

        outs = (s1, s2, s3_all, s4_all, s5)
        ins = (s1_in, s2_in, s3_in, s4_in, s5_in)

        def keep():
            return pltpu.make_async_copy(own, mine, own_sem.at[slot])

        if stage == 0:
            wait_own()
            keep().start()
        else:
            for d in outs[stage - 1]():
                d.wait_send()
            for d in ins[stage - 1]():
                d.wait_recv()
            if stage == 2:
                keep().wait()
        if stage < 5:
            for d in outs[stage]():
                d.start()

    def run_stage(stage, p):
        slot = lax.rem(p, SLOTS)

        @pl.when(p == 0)
        def _():
            stage_op(stage, wl_g, gath_g, wl_g.shape[0], SLOTS,
                     lambda: pltpu.make_async_copy(wl_g, wl_g, load_sem.at[n_piece]).wait())

        @pl.when(jnp.logical_and(p >= 0, p < first_d))
        def _():
            own = wl.at[p]
            stage_op(stage, own, gath.at[p], rows, slot,
                     lambda: pltpu.make_async_copy(own, own, load_sem.at[p]).wait())

        @pl.when(jnp.logical_and(p >= first_d, p < n_piece))
        def _():
            own = wl_d.at[p - first_d]
            stage_op(stage, own, gath_d.at[p - first_d], rows_d, slot,
                     lambda: pltpu.make_async_copy(own, own, load_sem.at[p]).wait())

    def tick(t):
        for stage in range(5):
            run_stage(stage, t - stage * LAG)
        run_stage(5, t - READY)

    def fetch(buf, dst, sem):
        cps = [pltpu.make_async_copy(buf.at[0], dst.at[:, :, 0], sem)]
        for y in range(side):
            cps.append(pltpu.make_async_copy(buf.at[1, :, y], dst.at[y, :, 1], sem))
        for cp in cps:
            cp.start()

    def fetch_piece(p):
        slot = lax.rem(p, 2)
        fetch(gath.at[p], wbuf.at[slot], wsem.at[slot])

    def wait_piece(p):
        slot = lax.rem(p, 2)
        pltpu.make_async_copy(wbuf.at[slot], wbuf.at[slot], wsem.at[slot]).wait()
        return slot

    def fetch_down(i):
        slot = lax.rem(i, 2)
        fetch(gath_d.at[i], wbuf_d.at[slot], wsem.at[2 + slot])

    def wait_down(i):
        slot = lax.rem(i, 2)
        pltpu.make_async_copy(wbuf_d.at[slot], wbuf_d.at[slot], wsem.at[2 + slot]).wait()
        return slot

    def row_loop(body, block=rb):
        def step(i, carry):
            body(pl.ds(pl.multiple_of(i * block, block), block))
            return carry

        lax.fori_loop(0, seq // block, step, 0)

    def norm_rows(src, dst, gain_row):
        nb = min(64, seq)

        def body(rs):
            xx = src[rs, :].astype(F32)
            scale = lax.rsqrt(jnp.mean(xx * xx, axis=-1, keepdims=True) + NORM_EPS)
            dst[rs, :] = ((xx * scale) * gains[pl.ds(gain_row, 1), :]).astype(BF16)

        row_loop(body, nb)

    def weight(slot):
        return wbuf[slot].reshape(dim, width)

    lane = lax.broadcasted_iota(jnp.int32, (rb, 128), 1)
    low_half = lax.rem(lane, cfg["head"]) < cfg["head"] // 2

    def rope(block, rs):
        up = block.astype(BF16).astype(F32)
        swapped = jnp.where(low_half, pltpu.roll(up, 128 - cfg["head"] // 2, 1), pltpu.roll(up, cfg["head"] // 2, 1))
        return up * cosv[rs, :] + swapped * sinv[rs, :]

    n_kv = kv_dim // cfg["head"]
    head = cfg["head"]
    col_v = (0, n_kv * 128)
    col_k = (2 * n_kv * 128, 2 * n_kv * 128 + seq)
    col_t = 2 * n_kv * 128 + 2 * seq

    def pre(t, carry):
        tick(t)
        return carry

    lax.fori_loop(0, READY + 1, pre, 0)
    fetch_piece(0)
    pltpu.sync_copy(gath_g, gvm)
    pltpu.make_async_copy(x_hbm, xv, misc_sem.at[0]).wait()
    pltpu.make_async_copy(cos_hbm, cost, misc_sem.at[1]).wait()
    pltpu.make_async_copy(sin_hbm, sint, misc_sem.at[2]).wait()
    for k in range(seq // tb):
        cc, ss = cost[:, k * tb:(k + 1) * tb], sint[:, k * tb:(k + 1) * tb]
        cosv[k * tb:(k + 1) * tb, :] = jnp.transpose(jnp.concatenate([cc] * 4, axis=0))
        sinv[k * tb:(k + 1) * tb, :] = jnp.transpose(jnp.concatenate([-ss, ss] * 2, axis=0))

    lane8 = lax.broadcasted_iota(jnp.int32, (8, 128), 1)
    for y in range(side):
        for x in range(side):
            for which in range(2):
                even = gvm[0, y, x, 8 * which:8 * which + 8, :]
                odd = gvm[1, x, y, 8 * which:8 * which + 8, :]
                c = (y * side + x) * 128
                gains[8 * which:8 * which + 8, c:c + 128] = jnp.where(lane8 < 64, even, pltpu.roll(odd, 64, 1))
    norm_rows(xv, hbuf, 0)

    tick(READY + 1)
    fetch_piece(1)
    slot = wait_piece(0)

    def kv_block(rs):
        acc = jnp.dot(hbuf[rs, :], weight(slot), preferred_element_type=F32)
        first = lane < head
        for c in range(kv_dim // 128):
            kr = rope(acc[:, c * 128:(c + 1) * 128], rs)
            kt = jnp.transpose(kr).astype(BF16)
            rbuf[c * 128:(c + 1) * 128, pl.ds(col_t + rs.start, rs.size)] = kt
            zero = jnp.zeros((head, rs.size), BF16)
            for g in range(2):
                kk = kt[g * head:(g + 1) * head]
                r0 = (2 * c + g) * 128
                rbuf[r0:r0 + head, pl.ds(col_k[0] + rs.start, rs.size)] = kk
                rbuf[r0 + head:r0 + 128, pl.ds(col_k[0] + rs.start, rs.size)] = zero
                rbuf[r0:r0 + head, pl.ds(col_k[1] + rs.start, rs.size)] = zero
                rbuf[r0 + head:r0 + 128, pl.ds(col_k[1] + rs.start, rs.size)] = kk
            vv = acc[:, kv_dim + c * 128:kv_dim + (c + 1) * 128]
            vt = jnp.transpose(vv).astype(BF16)
            rbuf[kv_dim + c * 128:kv_dim + (c + 1) * 128, pl.ds(col_t + rs.start, rs.size)] = vt
            turned = pltpu.roll(vv, head, 1)
            g0, g1 = 2 * c, 2 * c + 1
            rbuf[rs, col_v[0] + g0 * 128:col_v[0] + g0 * 128 + 128] = jnp.where(first, vv, 0.0).astype(BF16)
            rbuf[rs, col_v[1] + g0 * 128:col_v[1] + g0 * 128 + 128] = jnp.where(first, 0.0, turned).astype(BF16)
            rbuf[rs, col_v[0] + g1 * 128:col_v[0] + g1 * 128 + 128] = jnp.where(first, turned, 0.0).astype(BF16)
            rbuf[rs, col_v[1] + g1 * 128:col_v[1] + g1 * 128 + 128] = jnp.where(first, 0.0, vv).astype(BF16)

    row_loop(kv_block)
    kt_out = pltpu.make_async_copy(rbuf.at[pl.ds(0, kv_dim), pl.ds(col_t, seq)], kt_hbm, out_sem.at[n_down])
    vt_out = pltpu.make_async_copy(rbuf.at[pl.ds(kv_dim, kv_dim), pl.ds(col_t, seq)], vt_hbm, out_sem.at[n_down + 1])
    kt_out.start()
    vt_out.start()

    def q_step(c, carry):
        tick(READY + 2 + c)
        fetch_piece(2 + c)
        slot = wait_piece(1 + c)

        def q_block(rs):
            acc = jnp.dot(hbuf[rs, :], weight(slot), preferred_element_type=F32)
            for k in range(width // 128):
                dst = pl.ds(pl.multiple_of(c * width + k * 128, 128), 128)
                qbuf[rs, dst] = rope(acc[:, k * 128:(k + 1) * 128], rs).astype(BF16)

        row_loop(q_block)
        return carry

    lax.fori_loop(0, n_q, q_step, 0)
    t_now = READY + 2 + n_q

    n_pair = cfg["q_dim"] // 128
    pairs_per_kv = n_pair // n_kv
    qb = seq // len(ATTN_TICKS)
    scale = math.log2(math.e) * head ** -0.5
    causal = lax.broadcasted_iota(jnp.int32, (qb, qb), 0) >= lax.broadcasted_iota(jnp.int32, (qb, qb), 1)
    for i, n_t in enumerate(ATTN_TICKS):
        past = i * qb
        per = n_pair // n_t

        def one_pair(pi, i=i, past=past):
            g = pi // pairs_per_kv
            cs = pl.ds(pl.multiple_of(pi * 128, 128), 128)
            qp = qbuf[i * qb:(i + 1) * qb, cs]
            krow = pl.ds(pl.multiple_of(g * 128, 128), 128)
            total = None
            for hf in range(2):
                s_d = jnp.dot(qp, rbuf[krow, col_k[hf] + past:col_k[hf] + past + qb], preferred_element_type=F32)
                s_d = jnp.where(causal, s_d, -jnp.inf)
                m = jnp.max(s_d, axis=-1, keepdims=True)
                if past:
                    s_p = jnp.dot(qp, rbuf[krow, col_k[hf]:col_k[hf] + past], preferred_element_type=F32)
                    m = jnp.maximum(m, jnp.max(s_p, axis=-1, keepdims=True))
                e_d = jnp.exp2((s_d - m) * scale)
                den = jnp.sum(e_d, axis=-1, keepdims=True)
                if past:
                    e_p = jnp.exp2((s_p - m) * scale)
                    den = den + jnp.sum(e_p, axis=-1, keepdims=True)
                inv = 1.0 / den
                vcol = pl.ds(pl.multiple_of(col_v[hf] + g * 128, 128), 128)
                o = jnp.dot((e_d * inv).astype(BF16), rbuf[past:past + qb, vcol], preferred_element_type=F32)
                if past:
                    o = o + jnp.dot((e_p * inv).astype(BF16), rbuf[0:past, vcol], preferred_element_type=F32)
                total = o if total is None else total + o
            hbuf[i * qb:(i + 1) * qb, cs] = total.astype(BF16)

        def att_step(k, carry, one_pair=one_pair, per=per, base=t_now):
            tick(base + k)

            def inner(j, c2):
                one_pair(k * per + j)
                return c2

            lax.fori_loop(0, per, inner, 0)
            return carry

        lax.fori_loop(0, n_t, att_step, 0)
        t_now += n_t

    def o_step(c, carry):
        tick(t_now + c)
        fetch_piece(first_o + 1 + c)
        slot = wait_piece(first_o + c)

        def o_block(rs):
            acc = jnp.dot(hbuf[rs, :], weight(slot), preferred_element_type=F32)
            cs = pl.ds(pl.multiple_of(c * width, width), width)
            xv[rs, cs] = (xv[rs, cs].astype(F32) + acc.astype(BF16).astype(F32)).astype(BF16)

        row_loop(o_block)
        return carry

    lax.fori_loop(0, n_o, o_step, 0)
    t_now += n_o
    kt_out.wait()
    vt_out.wait()
    norm_rows(xv, qbuf, 8)

    def f_step(j, carry):
        @pl.when(lax.rem(j, 2) == 0)
        def _():
            tick(t_now + j // 2)

        @pl.when(j + 1 < n_ffn)
        def _():
            fetch_piece(first_f + j + 1)

        @pl.when(j + 1 == n_ffn)
        def _():
            fetch_down(0)

        slot = wait_piece(first_f + j)

        def f_block(rs):
            acc = jnp.dot(qbuf[rs, :], weight(slot), preferred_element_type=F32)
            gate = acc[:, :half_w].astype(BF16).astype(F32)
            up = acc[:, half_w:].astype(BF16).astype(F32)
            cs = pl.ds(pl.multiple_of(j * half_w, half_w), half_w)
            rbuf[rs, cs] = (jax.nn.silu(gate) * up).astype(BF16)

        row_loop(f_block)
        return carry

    lax.fori_loop(0, n_ffn, f_step, 0)
    t_now += (n_ffn + 1) // 2

    t_left = n_piece + READY - t_now
    skip = n_down - 1 - t_left

    def out_copy(i):
        cs = pl.ds(pl.multiple_of(i * width_d, width_d), width_d)
        return pltpu.make_async_copy(xv.at[:, cs], out_hbm.at[:, cs], out_sem.at[i])

    def d_step(i, carry):
        @pl.when(i < skip)
        def _():
            fetch_down(i + 1)

        slot = wait_down(i)
        cs = pl.ds(pl.multiple_of(i * width_d, width_d), width_d)

        def d_block(rs):
            acc = jnp.dot(rbuf[rs, :], wbuf_d[slot].reshape(ffn, width_d), preferred_element_type=F32)
            xv[rs, cs] = (xv[rs, cs].astype(F32) + acc.astype(BF16).astype(F32)).astype(BF16)

        row_loop(d_block)
        out_copy(i).start()

        @pl.when(jnp.logical_and(i >= skip, i < n_down - 1))
        def _():
            tick(t_now + i - skip)
            fetch_down(i + 1)

        return carry

    lax.fori_loop(0, n_down, d_step, 0)

    def finish(i, carry):
        out_copy(i).wait()
        return carry

    lax.fori_loop(0, n_down, finish, 0)
    assert skip >= 0 and sum(ATTN_TICKS) - skip <= n_down


def copy_kernel(a, b, c, a_out, b_out, c_out):
    a_out[...] = a[...]
    b_out[...] = b[...]
    c_out[...] = c[...]


def fresh_copy(a, b, c, steps=4):
    specs = [pl.BlockSpec((t.shape[0] // steps, t.shape[1]), lambda i: (i, 0)) for t in (a, b, c)]
    return pl.pallas_call(
        copy_kernel, grid=(steps,), in_specs=specs, out_specs=specs,
        out_shape=[jax.ShapeDtypeStruct(t.shape, t.dtype) for t in (a, b, c)])(a, b, c)


def solution(mesh, width=1024, width_d=256):
    n_dev = mesh.shape["fsdp"]
    side = math.isqrt(n_dev // 2)
    tok_spec = P(("dp", "fsdp"), None, None)
    cache_spec = P(("dp", "fsdp"), None, None, None)
    row_spec = P("fsdp", None)
    gain_spec = P("fsdp")
    table_spec = P(None, None)

    def local_layer(hidden, g_attn, w_query, w_key, w_value, w_out, g_mlp, w_gate, w_up, w_down, cos_tab, sin_tab):
        _, seq, dim = hidden.shape
        rows, q_dim = w_query.shape
        kv_dim = w_key.shape[1]
        ffn = w_gate.shape[1]
        rows_d = w_down.shape[0]
        head = 2 * cos_tab.shape[1]
        cfg = dict(side=side, seq=seq, dim=dim, ffn=ffn, width=width, width_d=width_d, kv_dim=kv_dim, q_dim=q_dim,
                   rows=rows, rows_d=rows_d, head=head)
        assert 2 * kv_dim == width and rows == 64 and rows * n_dev == dim
        both = jnp.stack([g_attn, g_mlp]).astype(F32)
        gain_tile = jnp.broadcast_to(jnp.pad(both, ((0, 0), (0, 128 - rows)))[:, None, :], (2, 8, 128)).reshape(16, 128)
        n_wide = (2 * kv_dim + q_dim + dim + 2 * ffn) // width
        n_down = dim // width_d
        n_piece = n_wide + n_down
        hbm = pl.BlockSpec(memory_space=pl.ANY)
        res = pl.pallas_call(
            functools.partial(layer_kernel, cfg),
            out_shape=(
                jax.ShapeDtypeStruct((seq, dim), BF16),
                jax.ShapeDtypeStruct((kv_dim, seq), BF16),
                jax.ShapeDtypeStruct((kv_dim, seq), BF16),
                jax.ShapeDtypeStruct((n_wide, 2, side, side, rows, width), BF16),
                jax.ShapeDtypeStruct((n_down, 2, side, side, rows_d, width_d), BF16),
                jax.ShapeDtypeStruct((2, side, side, 16, 128), F32)),
            in_specs=[hbm] * 11,
            out_specs=[hbm] * 6,
            scratch_shapes=[
                pltpu.VMEM((seq, dim), BF16),
                pltpu.VMEM((seq, max(dim, q_dim)), BF16),
                pltpu.VMEM((seq, max(dim, q_dim)), BF16),
                pltpu.VMEM((max(seq, 2 * kv_dim), ffn), BF16),
                pltpu.VMEM((2, side, side, 2, rows, width), BF16),
                pltpu.VMEM((2, side, side, 2, rows_d, width_d), BF16),
                pltpu.VMEM((n_wide, rows, width), BF16),
                pltpu.VMEM((n_down, rows_d, width_d), BF16),
                pltpu.VMEM((16, 128), F32),
                pltpu.VMEM((2, side, side, 16, 128), F32),
                pltpu.VMEM((16, dim), F32),
                pltpu.VMEM((seq, 128), F32),
                pltpu.VMEM((seq, 128), F32),
                pltpu.VMEM((head // 2, seq), F32),
                pltpu.VMEM((head // 2, seq), F32),
                pltpu.SemaphoreType.DMA((6, 2, SLOTS + 1)),
                pltpu.SemaphoreType.DMA((6, 2, SLOTS + 1)),
                pltpu.SemaphoreType.DMA((SLOTS + 1,)),
                pltpu.SemaphoreType.DMA((n_piece + 1,)),
                pltpu.SemaphoreType.DMA((4,)),
                pltpu.SemaphoreType.DMA((3,)),
                pltpu.SemaphoreType.DMA((n_down + 2,)),
            ],
            compiler_params=pltpu.CompilerParams(
                collective_id=0, has_side_effects=True, vmem_limit_bytes=67043328),
        )(hidden[0], gain_tile, w_query, w_key, w_value, w_out, w_gate, w_up, w_down, cos_tab.T, sin_tab.T)
        out, kt, vt = fresh_copy(*res[:3])

        def cache(t):
            return jnp.transpose(t.reshape(1, kv_dim // head, head, seq), (0, 3, 1, 2))

        return out[None], cache(kt), cache(vt)

    return jax.shard_map(local_layer, mesh=mesh, in_specs=(tok_spec, gain_spec, row_spec, row_spec, row_spec, row_spec, gain_spec, row_spec, row_spec, row_spec, table_spec, table_spec), out_specs=(tok_spec, cache_spec, cache_spec), check_vma=False)
```

```python
import functools
import math
import jax
import jax.numpy as jnp
from jax import lax
from jax.experimental import pallas as pl
from jax.experimental.pallas import tpu as pltpu
from jax.sharding import PartitionSpec as P

NORM_EPS = 1e-5
MESH = pl.DeviceIdType.MESH
LAG = 2
SLOTS = 2 * LAG + 4
READY = 4 * LAG + 1
ATTN_TICKS = (1, 1, 2, 2)
FFN_PAIRED = 13
ROW_BLOCK = 256
BF16 = jnp.bfloat16
F32 = jnp.float32


def layer_kernel(cfg, x_hbm, gain_hbm, wq, wk, wv, wo, wg, wu, wd, cos_hbm, sin_hbm,
                 out_hbm, kt_hbm, vt_hbm, gath, gath_d, gath_g,
                 xv, hbuf, qbuf, rbuf, wbuf, wbuf_d, wl, wl_d, wl_g, gvm, gains, cosv, sinv, cost, sint,
                 send_sem, recv_sem, own_sem, load_sem, wsem, misc_sem, out_sem):
    side, seq, dim, ffn = cfg["side"], cfg["seq"], cfg["dim"], cfg["ffn"]
    width, half_w, width_d = cfg["width"], cfg["width"] // 2, cfg["width_d"]
    kv_dim = cfg["kv_dim"]
    n_q, n_o = cfg["q_dim"] // width, dim // width
    n_ffn, n_down = ffn // half_w, dim // width_d
    first_o = 1 + n_q
    first_f = first_o + n_o
    first_d = first_f + n_ffn
    n_piece = first_d + n_down
    rows, rows_d = cfg["rows"], cfg["rows_d"]
    rb = min(ROW_BLOCK, seq)
    tb = min(128, seq)

    me = lax.axis_index("fsdp")
    core = lax.rem(me, 2)
    px = lax.rem(me // 2, side)
    py = me // (2 * side)
    pa = px + core * (py - px)
    pb = py + core * (px - py)
    a_up, a_dn = lax.rem(pa + 1, side), lax.rem(pa + side - 1, side)
    b_up, b_dn = lax.rem(pb + 1, side), lax.rem(pb + side - 1, side)

    def device_at(a, b):
        y = b + core * (a - b)
        x = a + core * (b - a)
        return (y * side + x) * 2 + core

    dev_ap, dev_am = device_at(a_up, pb), device_at(a_dn, pb)
    dev_bp, dev_bm = device_at(pa, b_up), device_at(pa, b_dn)
    sibling = me + 1 - 2 * core

    def load(src, dst, sem):
        pltpu.make_async_copy(src, dst, sem).start()

    load(gain_hbm, wl_g, load_sem.at[n_piece])
    load(wk, wl.at[0, :, pl.ds(0, kv_dim)], load_sem.at[0])
    load(wv, wl.at[0, :, pl.ds(kv_dim, kv_dim)], load_sem.at[0])
    for c in range(n_q):
        load(wq.at[:, pl.ds(c * width, width)], wl.at[1 + c], load_sem.at[1 + c])
    load(x_hbm, xv, misc_sem.at[0])
    load(cos_hbm, cost, misc_sem.at[1])
    load(sin_hbm, sint, misc_sem.at[2])
    for c in range(n_o):
        load(wo.at[:, pl.ds(c * width, width)], wl.at[first_o + c], load_sem.at[first_o + c])

    def load_ffn(j, carry):
        col = pl.multiple_of(j * half_w, half_w)
        load(wg.at[:, pl.ds(col, half_w)], wl.at[first_f + j, :, pl.ds(0, half_w)], load_sem.at[first_f + j])
        load(wu.at[:, pl.ds(col, half_w)], wl.at[first_f + j, :, pl.ds(half_w, half_w)], load_sem.at[first_f + j])
        return carry

    lax.fori_loop(0, n_ffn, load_ffn, 0)

    def load_down(j, carry):
        col = pl.multiple_of(j * width_d, width_d)
        load(wd.at[:, pl.ds(col, width_d)], wl_d.at[j], load_sem.at[first_d + j])
        return carry

    lax.fori_loop(0, n_down, load_down, 0)

    dp = lax.axis_index("dp")
    barrier = pltpu.get_barrier_semaphore()
    for peer in (dev_ap, dev_am, dev_bp, dev_bm, sibling):
        pl.semaphore_signal(barrier, inc=1, device_id=(dp, peer), device_id_type=MESH)
    pl.semaphore_wait(barrier, 5)

    def remote(src, dst, stage, way, slot, peer):
        return pltpu.make_async_remote_copy(
            src_ref=src, dst_ref=dst, send_sem=send_sem.at[stage, way, slot], recv_sem=recv_sem.at[stage, way, slot],
            device_id=(dp, peer), device_id_type=MESH)

    def stage_op(stage, own, buf, n_rows, slot, wait_own):
        h = n_rows // 2
        mine = buf.at[core, pb, pa]

        def s1():
            return (remote(own, mine, 0, 0, slot, dev_ap), remote(own, mine, 0, 1, slot, dev_am))

        def s1_in():
            lo, hi = buf.at[core, pb, a_dn], buf.at[core, pb, a_up]
            return (remote(lo, lo, 0, 0, slot, dev_ap), remote(hi, hi, 0, 1, slot, dev_am))

        def s2():
            lo, hi = buf.at[core, pb, a_dn, pl.ds(0, h)], buf.at[core, pb, a_up, pl.ds(h, h)]
            return (remote(lo, lo, 1, 0, slot, dev_ap), remote(hi, hi, 1, 1, slot, dev_am))

        def s2_in():
            far = lax.rem(pa + 2, side)
            lo, hi = buf.at[core, pb, far, pl.ds(0, h)], buf.at[core, pb, far, pl.ds(h, h)]
            return (remote(lo, lo, 1, 0, slot, dev_ap), remote(hi, hi, 1, 1, slot, dev_am))

        def s3():
            line = buf.at[core, pb]
            return (remote(line, line, 2, 0, slot, dev_bp), remote(line, line, 2, 1, slot, dev_bm))

        def s3_in():
            lo, hi = buf.at[core, b_dn], buf.at[core, b_up]
            return (remote(lo, lo, 2, 0, slot, dev_bp), remote(hi, hi, 2, 1, slot, dev_bm))

        def s4():
            lo, hi = buf.at[core, b_dn, pl.ds(0, side // 2)], buf.at[core, b_up, pl.ds(side // 2, side // 2)]
            return (remote(lo, lo, 3, 0, slot, dev_bp), remote(hi, hi, 3, 1, slot, dev_bm))

        def s4_in():
            far = lax.rem(pb + 2, side)
            lo, hi = buf.at[core, far, pl.ds(0, side // 2)], buf.at[core, far, pl.ds(side // 2, side // 2)]
            return (remote(lo, lo, 3, 0, slot, dev_bp), remote(hi, hi, 3, 1, slot, dev_bm))

        def hand(line, row, way):
            ref = buf.at[core, line]
            return remote(ref, ref, row, way, slot, sibling)

        def hand_in(line, row, way):
            ref = buf.at[1 - core, line]
            return remote(ref, ref, row, way, slot, sibling)

        def s3_all():
            return s3() + (hand(pb, 4, 0),)

        def s4_all():
            return s4() + (hand(b_dn, 4, 1), hand(b_up, 5, 0))

        def s5():
            return (hand(lax.rem(pb + 2, side), 5, 1),)

        def s5_in():
            return (hand_in(pa, 4, 0), hand_in(a_dn, 4, 1), hand_in(a_up, 5, 0), hand_in(lax.rem(pa + 2, side), 5, 1))

        outs = (s1, s2, s3_all, s4_all, s5)
        ins = (s1_in, s2_in, s3_in, s4_in, s5_in)

        def keep():
            return pltpu.make_async_copy(own, mine, own_sem.at[slot])

        if stage == 0:
            wait_own()
            keep().start()
        else:
            for d in outs[stage - 1]():
                d.wait_send()
            for d in ins[stage - 1]():
                d.wait_recv()
            if stage == 2:
                keep().wait()
        if stage < 5:
            for d in outs[stage]():
                d.start()

    def run_stage(stage, p):
        slot = lax.rem(p, SLOTS)

        @pl.when(p == 0)
        def _():
            stage_op(stage, wl_g, gath_g, wl_g.shape[0], SLOTS,
                     lambda: pltpu.make_async_copy(wl_g, wl_g, load_sem.at[n_piece]).wait())

        @pl.when(jnp.logical_and(p >= 0, p < first_d))
        def _():
            own = wl.at[p]
            stage_op(stage, own, gath.at[p], rows, slot,
                     lambda: pltpu.make_async_copy(own, own, load_sem.at[p]).wait())

        @pl.when(jnp.logical_and(p >= first_d, p < n_piece))
        def _():
            own = wl_d.at[p - first_d]
            stage_op(stage, own, gath_d.at[p - first_d], rows_d, slot,
                     lambda: pltpu.make_async_copy(own, own, load_sem.at[p]).wait())

    def tick(t):
        for stage in range(5):
            run_stage(stage, t - stage * LAG)
        run_stage(5, t - READY)

    def fetch(buf, dst, sem):
        cps = [pltpu.make_async_copy(buf.at[0], dst.at[:, :, 0], sem)]
        for y in range(side):
            cps.append(pltpu.make_async_copy(buf.at[1, :, y], dst.at[y, :, 1], sem))
        for cp in cps:
            cp.start()

    def fetch_piece(p):
        slot = lax.rem(p, 2)
        fetch(gath.at[p], wbuf.at[slot], wsem.at[slot])

    def wait_piece(p):
        slot = lax.rem(p, 2)
        pltpu.make_async_copy(wbuf.at[slot], wbuf.at[slot], wsem.at[slot]).wait()
        return slot

    def fetch_down(i):
        slot = lax.rem(i, 2)
        fetch(gath_d.at[i], wbuf_d.at[slot], wsem.at[2 + slot])

    def wait_down(i):
        slot = lax.rem(i, 2)
        pltpu.make_async_copy(wbuf_d.at[slot], wbuf_d.at[slot], wsem.at[2 + slot]).wait()
        return slot

    def row_loop(body, block=rb):
        def step(i, carry):
            body(pl.ds(pl.multiple_of(i * block, block), block))
            return carry

        lax.fori_loop(0, seq // block, step, 0)

    def norm_rows(src, dst, gain_row):
        nb = min(64, seq)

        def body(rs):
            xx = src[rs, :].astype(F32)
            scale = lax.rsqrt(jnp.mean(xx * xx, axis=-1, keepdims=True) + NORM_EPS)
            dst[rs, :] = ((xx * scale) * gains[pl.ds(gain_row, 1), :]).astype(BF16)

        row_loop(body, nb)

    def weight(slot):
        return wbuf[slot].reshape(dim, width)

    lane = lax.broadcasted_iota(jnp.int32, (rb, 128), 1)
    low_half = lax.rem(lane, cfg["head"]) < cfg["head"] // 2

    def rope(block, rs):
        up = block.astype(BF16).astype(F32)
        swapped = jnp.where(low_half, pltpu.roll(up, 128 - cfg["head"] // 2, 1), pltpu.roll(up, cfg["head"] // 2, 1))
        return up * cosv[rs, :] + swapped * sinv[rs, :]

    n_kv = kv_dim // cfg["head"]
    head = cfg["head"]
    col_v = (0, n_kv * 128)
    col_k = (2 * n_kv * 128, 2 * n_kv * 128 + seq)
    col_t = 2 * n_kv * 128 + 2 * seq

    def pre(t, carry):
        tick(t)
        return carry

    lax.fori_loop(0, LAG + 1, pre, 0)
    pltpu.make_async_copy(cos_hbm, cost, misc_sem.at[1]).wait()
    pltpu.make_async_copy(sin_hbm, sint, misc_sem.at[2]).wait()
    for k in range(seq // tb):
        cc, ss = cost[:, k * tb:(k + 1) * tb], sint[:, k * tb:(k + 1) * tb]
        cosv[k * tb:(k + 1) * tb, :] = jnp.transpose(jnp.concatenate([cc] * 4, axis=0))
        sinv[k * tb:(k + 1) * tb, :] = jnp.transpose(jnp.concatenate([-ss, ss] * 2, axis=0))
    lax.fori_loop(LAG + 1, READY + 1, pre, 0)
    fetch_piece(0)
    pltpu.sync_copy(gath_g, gvm)
    pltpu.make_async_copy(x_hbm, xv, misc_sem.at[0]).wait()
    lane8 = lax.broadcasted_iota(jnp.int32, (8, 128), 1)
    for y in range(side):
        for x in range(side):
            for which in range(2):
                even = gvm[0, y, x, 8 * which:8 * which + 8, :]
                odd = gvm[1, x, y, 8 * which:8 * which + 8, :]
                c = (y * side + x) * 128
                gains[8 * which:8 * which + 8, c:c + 128] = jnp.where(lane8 < 64, even, pltpu.roll(odd, 64, 1))
    norm_rows(xv, hbuf, 0)

    slot = wait_piece(0)

    def kv_block(rs):
        acc = jnp.dot(hbuf[rs, :], weight(slot), preferred_element_type=F32)
        first = lane < head
        for c in range(kv_dim // 128):
            kr = rope(acc[:, c * 128:(c + 1) * 128], rs)
            kt = jnp.transpose(kr).astype(BF16)
            rbuf[c * 128:(c + 1) * 128, pl.ds(col_t + rs.start, rs.size)] = kt
            zero = jnp.zeros((head, rs.size), BF16)
            for g in range(2):
                kk = kt[g * head:(g + 1) * head]
                r0 = (2 * c + g) * 128
                rbuf[r0:r0 + head, pl.ds(col_k[0] + rs.start, rs.size)] = kk
                rbuf[r0 + head:r0 + 128, pl.ds(col_k[0] + rs.start, rs.size)] = zero
                rbuf[r0:r0 + head, pl.ds(col_k[1] + rs.start, rs.size)] = zero
                rbuf[r0 + head:r0 + 128, pl.ds(col_k[1] + rs.start, rs.size)] = kk
            vv = acc[:, kv_dim + c * 128:kv_dim + (c + 1) * 128]
            vt = jnp.transpose(vv).astype(BF16)
            rbuf[kv_dim + c * 128:kv_dim + (c + 1) * 128, pl.ds(col_t + rs.start, rs.size)] = vt
            turned = pltpu.roll(vv, head, 1)
            g0, g1 = 2 * c, 2 * c + 1
            rbuf[rs, col_v[0] + g0 * 128:col_v[0] + g0 * 128 + 128] = jnp.where(first, vv, 0.0).astype(BF16)
            rbuf[rs, col_v[1] + g0 * 128:col_v[1] + g0 * 128 + 128] = jnp.where(first, 0.0, turned).astype(BF16)
            rbuf[rs, col_v[0] + g1 * 128:col_v[0] + g1 * 128 + 128] = jnp.where(first, turned, 0.0).astype(BF16)
            rbuf[rs, col_v[1] + g1 * 128:col_v[1] + g1 * 128 + 128] = jnp.where(first, 0.0, vv).astype(BF16)

    row_loop(kv_block)
    kt_out = pltpu.make_async_copy(rbuf.at[pl.ds(0, kv_dim), pl.ds(col_t, seq)], kt_hbm, out_sem.at[n_down])
    vt_out = pltpu.make_async_copy(rbuf.at[pl.ds(kv_dim, kv_dim), pl.ds(col_t, seq)], vt_hbm, out_sem.at[n_down + 1])
    kt_out.start()
    vt_out.start()

    def q_step(c, carry):
        tick(READY + 1 + c)
        fetch_piece(1 + c)
        slot = wait_piece(1 + c)

        def q_block(rs):
            acc = jnp.dot(hbuf[rs, :], weight(slot), preferred_element_type=F32)
            for k in range(width // 128):
                dst = pl.ds(pl.multiple_of(c * width + k * 128, 128), 128)
                qbuf[rs, dst] = rope(acc[:, k * 128:(k + 1) * 128], rs).astype(BF16)

        row_loop(q_block)
        return carry

    lax.fori_loop(0, n_q, q_step, 0)
    t_now = READY + 1 + n_q

    n_pair = cfg["q_dim"] // 128
    pairs_per_kv = n_pair // n_kv
    qb = seq // len(ATTN_TICKS)
    scale = math.log2(math.e) * head ** -0.5
    causal = lax.broadcasted_iota(jnp.int32, (qb, qb), 0) >= lax.broadcasted_iota(jnp.int32, (qb, qb), 1)
    for i, n_t in enumerate(ATTN_TICKS):
        past = i * qb
        per = n_pair // n_t

        def one_pair(pi, i=i, past=past):
            g = pi // pairs_per_kv
            cs = pl.ds(pl.multiple_of(pi * 128, 128), 128)
            qp = qbuf[i * qb:(i + 1) * qb, cs]
            krow = pl.ds(pl.multiple_of(g * 128, 128), 128)
            total = None
            for hf in range(2):
                s_d = jnp.dot(qp, rbuf[krow, col_k[hf] + past:col_k[hf] + past + qb], preferred_element_type=F32)
                s_d = jnp.where(causal, s_d, -jnp.inf)
                m = jnp.max(s_d, axis=-1, keepdims=True)
                if past:
                    s_p = jnp.dot(qp, rbuf[krow, col_k[hf]:col_k[hf] + past], preferred_element_type=F32)
                    m = jnp.maximum(m, jnp.max(s_p, axis=-1, keepdims=True))
                e_d = jnp.exp2((s_d - m) * scale)
                den = jnp.sum(e_d, axis=-1, keepdims=True)
                if past:
                    e_p = jnp.exp2((s_p - m) * scale)
                    den = den + jnp.sum(e_p, axis=-1, keepdims=True)
                inv = 1.0 / den
                vcol = pl.ds(pl.multiple_of(col_v[hf] + g * 128, 128), 128)
                o = jnp.dot((e_d * inv).astype(BF16), rbuf[past:past + qb, vcol], preferred_element_type=F32)
                if past:
                    o = o + jnp.dot((e_p * inv).astype(BF16), rbuf[0:past, vcol], preferred_element_type=F32)
                total = o if total is None else total + o
            hbuf[i * qb:(i + 1) * qb, cs] = total.astype(BF16)

        def att_step(k, carry, one_pair=one_pair, per=per, base=t_now):
            tick(base + k)

            def inner(j, c2):
                one_pair(k * per + j)
                return c2

            lax.fori_loop(0, per, inner, 0)
            return carry

        lax.fori_loop(0, n_t, att_step, 0)
        t_now += n_t
        if i == 0:
            fetch_piece(first_o)

    def o_step(c, carry):
        tick(t_now + c)
        fetch_piece(first_o + 1 + c)
        slot = wait_piece(first_o + c)

        def o_block(rs):
            acc = jnp.dot(hbuf[rs, :], weight(slot), preferred_element_type=F32)
            cs = pl.ds(pl.multiple_of(c * width, width), width)
            xv[rs, cs] = (xv[rs, cs].astype(F32) + acc.astype(BF16).astype(F32)).astype(BF16)

        row_loop(o_block)
        return carry

    lax.fori_loop(0, n_o, o_step, 0)
    t_now += n_o
    kt_out.wait()
    vt_out.wait()
    norm_rows(xv, qbuf, 8)

    ticks_by = [min(j, FFN_PAIRED) // 2 + (j < FFN_PAIRED) + max(0, j - FFN_PAIRED + 1) + (j >= FFN_PAIRED) * (FFN_PAIRED % 2)
                for j in range(n_ffn)]
    early = [t_now - 1 + ticks_by[j] - READY >= first_f + j + 1 and j + 1 < n_ffn for j in range(n_ffn)]
    n_early = sum(early)
    assert all(early[:n_early]) and all(t_now - 1 + ticks_by[j] - READY >= first_f + j for j in range(n_ffn))

    def f_step(j, carry):
        @pl.when(jnp.logical_and(lax.rem(j, 2) == 0, j < FFN_PAIRED))
        def _():
            tick(t_now + j // 2)

        @pl.when(j >= FFN_PAIRED)
        def _():
            tick(t_now + (FFN_PAIRED + 1) // 2 + j - FFN_PAIRED)

        @pl.when(j > n_early)
        def _():
            fetch_piece(first_f + j)

        @pl.when(j < n_early)
        def _():
            fetch_piece(first_f + j + 1)

        slot = wait_piece(first_f + j)

        def f_block(rs):
            acc = jnp.dot(qbuf[rs, :], weight(slot), preferred_element_type=F32)
            gate = acc[:, :half_w].astype(BF16).astype(F32)
            up = acc[:, half_w:].astype(BF16).astype(F32)
            cs = pl.ds(pl.multiple_of(j * half_w, half_w), half_w)
            rbuf[rs, cs] = (jax.nn.silu(gate) * up).astype(BF16)

        row_loop(f_block)
        return carry

    lax.fori_loop(0, n_ffn, f_step, 0)
    t_now += ticks_by[-1]

    def out_copy(i):
        cs = pl.ds(pl.multiple_of(i * width_d, width_d), width_d)
        return pltpu.make_async_copy(xv.at[:, cs], out_hbm.at[:, cs], out_sem.at[i])

    def d_step(i, carry):
        tick(t_now + i)
        fetch_down(i)
        slot = wait_down(i)
        cs = pl.ds(pl.multiple_of(i * width_d, width_d), width_d)

        def d_block(rs):
            acc = jnp.dot(rbuf[rs, :], wbuf_d[slot].reshape(ffn, width_d), preferred_element_type=F32)
            xv[rs, cs] = (xv[rs, cs].astype(F32) + acc.astype(BF16).astype(F32)).astype(BF16)

        row_loop(d_block)
        out_copy(i).start()
        return carry

    lax.fori_loop(0, n_down, d_step, 0)

    def finish(i, carry):
        out_copy(i).wait()
        return carry

    lax.fori_loop(0, n_down, finish, 0)
    assert t_now + n_down >= n_piece + READY


def copy_kernel(a, b, c, a_out, b_out, c_out):
    a_out[...] = a[...]
    b_out[...] = b[...]
    c_out[...] = c[...]


def fresh_copy(a, b, c, steps=4):
    specs = [pl.BlockSpec((t.shape[0] // steps, t.shape[1]), lambda i: (i, 0)) for t in (a, b, c)]
    return pl.pallas_call(
        copy_kernel, grid=(steps,), in_specs=specs, out_specs=specs,
        out_shape=[jax.ShapeDtypeStruct(t.shape, t.dtype) for t in (a, b, c)])(a, b, c)


def solution(mesh, width=1024, width_d=256):
    n_dev = mesh.shape["fsdp"]
    side = math.isqrt(n_dev // 2)
    tok_spec = P(("dp", "fsdp"), None, None)
    cache_spec = P(("dp", "fsdp"), None, None, None)
    row_spec = P("fsdp", None)
    gain_spec = P("fsdp")
    table_spec = P(None, None)

    def local_layer(hidden, g_attn, w_query, w_key, w_value, w_out, g_mlp, w_gate, w_up, w_down, cos_tab, sin_tab):
        _, seq, dim = hidden.shape
        rows, q_dim = w_query.shape
        kv_dim = w_key.shape[1]
        ffn = w_gate.shape[1]
        rows_d = w_down.shape[0]
        head = 2 * cos_tab.shape[1]
        cfg = dict(side=side, seq=seq, dim=dim, ffn=ffn, width=width, width_d=width_d, kv_dim=kv_dim, q_dim=q_dim,
                   rows=rows, rows_d=rows_d, head=head)
        assert 2 * kv_dim == width and rows == 64 and rows * n_dev == dim
        both = jnp.stack([g_attn, g_mlp]).astype(F32)
        gain_tile = jnp.broadcast_to(jnp.pad(both, ((0, 0), (0, 128 - rows)))[:, None, :], (2, 8, 128)).reshape(16, 128)
        n_wide = (2 * kv_dim + q_dim + dim + 2 * ffn) // width
        n_down = dim // width_d
        n_piece = n_wide + n_down
        hbm = pl.BlockSpec(memory_space=pl.ANY)
        res = pl.pallas_call(
            functools.partial(layer_kernel, cfg),
            out_shape=(
                jax.ShapeDtypeStruct((seq, dim), BF16),
                jax.ShapeDtypeStruct((kv_dim, seq), BF16),
                jax.ShapeDtypeStruct((kv_dim, seq), BF16),
                jax.ShapeDtypeStruct((n_wide, 2, side, side, rows, width), BF16),
                jax.ShapeDtypeStruct((n_down, 2, side, side, rows_d, width_d), BF16),
                jax.ShapeDtypeStruct((2, side, side, 16, 128), F32)),
            in_specs=[hbm] * 11,
            out_specs=[hbm] * 6,
            scratch_shapes=[
                pltpu.VMEM((seq, dim), BF16),
                pltpu.VMEM((seq, max(dim, q_dim)), BF16),
                pltpu.VMEM((seq, max(dim, q_dim)), BF16),
                pltpu.VMEM((max(seq, 2 * kv_dim), ffn), BF16),
                pltpu.VMEM((2, side, side, 2, rows, width), BF16),
                pltpu.VMEM((2, side, side, 2, rows_d, width_d), BF16),
                pltpu.VMEM((n_wide, rows, width), BF16),
                pltpu.VMEM((n_down, rows_d, width_d), BF16),
                pltpu.VMEM((16, 128), F32),
                pltpu.VMEM((2, side, side, 16, 128), F32),
                pltpu.VMEM((16, dim), F32),
                pltpu.VMEM((seq, 128), F32),
                pltpu.VMEM((seq, 128), F32),
                pltpu.VMEM((head // 2, seq), F32),
                pltpu.VMEM((head // 2, seq), F32),
                pltpu.SemaphoreType.DMA((6, 2, SLOTS + 1)),
                pltpu.SemaphoreType.DMA((6, 2, SLOTS + 1)),
                pltpu.SemaphoreType.DMA((SLOTS + 1,)),
                pltpu.SemaphoreType.DMA((n_piece + 1,)),
                pltpu.SemaphoreType.DMA((4,)),
                pltpu.SemaphoreType.DMA((3,)),
                pltpu.SemaphoreType.DMA((n_down + 2,)),
            ],
            compiler_params=pltpu.CompilerParams(
                collective_id=0, has_side_effects=True, vmem_limit_bytes=67043328),
        )(hidden[0], gain_tile, w_query, w_key, w_value, w_out, w_gate, w_up, w_down, cos_tab.T, sin_tab.T)
        out, kt, vt = fresh_copy(*res[:3])

        def cache(t):
            return jnp.transpose(t.reshape(1, kv_dim // head, head, seq), (0, 3, 1, 2))

        return out[None], cache(kt), cache(vt)

    return jax.shard_map(local_layer, mesh=mesh, in_specs=(tok_spec, gain_spec, row_spec, row_spec, row_spec, row_spec, gain_spec, row_spec, row_spec, row_spec, table_spec, table_spec), out_specs=(tok_spec, cache_spec, cache_spec), check_vma=False)
```

```python
import functools
import math
import jax
import jax.numpy as jnp
from jax import lax
from jax.experimental import pallas as pl
from jax.experimental.pallas import tpu as pltpu
from jax.sharding import PartitionSpec as P

NORM_EPS = 1e-5
MESH = pl.DeviceIdType.MESH
LAG = 2
SLOTS = 2 * LAG + 4
READY = 4 * LAG + 1
ATTN_TICKS = (1, 1, 2, 2)
FFN_PAIRED = 13
ROW_BLOCK = 256
VMEM_MAIN = 38 << 20
BF16 = jnp.bfloat16
F32 = jnp.float32


def layer_kernel(cfg, x_hbm, gain_hbm, wq, wk, wv, wo, wg, wu, wd, cos_hbm, sin_hbm,
                 xv, rbuf, kt_out, vt_out, gath, gath_d, gath_g,
                 hbuf, qbuf, wbuf, wbuf_d, wl, wl_d, wl_g, gvm, gains, cosv, sinv, cost, sint,
                 send_sem, recv_sem, own_sem, load_sem, wsem, misc_sem):
    side, seq, dim, ffn = cfg["side"], cfg["seq"], cfg["dim"], cfg["ffn"]
    width, half_w, width_d = cfg["width"], cfg["width"] // 2, cfg["width_d"]
    kv_dim = cfg["kv_dim"]
    n_q, n_o = cfg["q_dim"] // width, dim // width
    n_ffn, n_down = ffn // half_w, dim // width_d
    first_o = 1 + n_q
    first_f = first_o + n_o
    first_d = first_f + n_ffn
    n_piece = first_d + n_down
    rows, rows_d = cfg["rows"], cfg["rows_d"]
    rb = min(ROW_BLOCK, seq)
    tb = min(128, seq)

    me = lax.axis_index("fsdp")
    core = lax.rem(me, 2)
    px = lax.rem(me // 2, side)
    py = me // (2 * side)
    pa = px + core * (py - px)
    pb = py + core * (px - py)
    a_up, a_dn = lax.rem(pa + 1, side), lax.rem(pa + side - 1, side)
    b_up, b_dn = lax.rem(pb + 1, side), lax.rem(pb + side - 1, side)

    def device_at(a, b):
        y = b + core * (a - b)
        x = a + core * (b - a)
        return (y * side + x) * 2 + core

    dev_ap, dev_am = device_at(a_up, pb), device_at(a_dn, pb)
    dev_bp, dev_bm = device_at(pa, b_up), device_at(pa, b_dn)
    sibling = me + 1 - 2 * core

    def load(src, dst, sem):
        pltpu.make_async_copy(src, dst, sem).start()

    load(gain_hbm, wl_g, load_sem.at[n_piece])
    load(wk, wl.at[0, :, pl.ds(0, kv_dim)], load_sem.at[0])
    load(wv, wl.at[0, :, pl.ds(kv_dim, kv_dim)], load_sem.at[0])
    for c in range(n_q):
        load(wq.at[:, pl.ds(c * width, width)], wl.at[1 + c], load_sem.at[1 + c])
    load(x_hbm, xv, misc_sem.at[0])
    load(cos_hbm, cost, misc_sem.at[1])
    load(sin_hbm, sint, misc_sem.at[2])
    for c in range(n_o):
        load(wo.at[:, pl.ds(c * width, width)], wl.at[first_o + c], load_sem.at[first_o + c])

    def load_ffn(j, carry):
        col = pl.multiple_of(j * half_w, half_w)
        load(wg.at[:, pl.ds(col, half_w)], wl.at[first_f + j, :, pl.ds(0, half_w)], load_sem.at[first_f + j])
        load(wu.at[:, pl.ds(col, half_w)], wl.at[first_f + j, :, pl.ds(half_w, half_w)], load_sem.at[first_f + j])
        return carry

    lax.fori_loop(0, n_ffn, load_ffn, 0)

    def load_down(j, carry):
        col = pl.multiple_of(j * width_d, width_d)
        load(wd.at[:, pl.ds(col, width_d)], wl_d.at[j], load_sem.at[first_d + j])
        return carry

    lax.fori_loop(0, n_down, load_down, 0)

    dp = lax.axis_index("dp")
    barrier = pltpu.get_barrier_semaphore()
    for peer in (dev_ap, dev_am, dev_bp, dev_bm, sibling):
        pl.semaphore_signal(barrier, inc=1, device_id=(dp, peer), device_id_type=MESH)
    pl.semaphore_wait(barrier, 5)

    def remote(src, dst, stage, way, slot, peer):
        return pltpu.make_async_remote_copy(
            src_ref=src, dst_ref=dst, send_sem=send_sem.at[stage, way, slot], recv_sem=recv_sem.at[stage, way, slot],
            device_id=(dp, peer), device_id_type=MESH)

    def stage_op(stage, own, buf, n_rows, slot, wait_own):
        h = n_rows // 2
        mine = buf.at[core, pb, pa]

        def s1():
            return (remote(own, mine, 0, 0, slot, dev_ap), remote(own, mine, 0, 1, slot, dev_am))

        def s1_in():
            lo, hi = buf.at[core, pb, a_dn], buf.at[core, pb, a_up]
            return (remote(lo, lo, 0, 0, slot, dev_ap), remote(hi, hi, 0, 1, slot, dev_am))

        def s2():
            lo, hi = buf.at[core, pb, a_dn, pl.ds(0, h)], buf.at[core, pb, a_up, pl.ds(h, h)]
            return (remote(lo, lo, 1, 0, slot, dev_ap), remote(hi, hi, 1, 1, slot, dev_am))

        def s2_in():
            far = lax.rem(pa + 2, side)
            lo, hi = buf.at[core, pb, far, pl.ds(0, h)], buf.at[core, pb, far, pl.ds(h, h)]
            return (remote(lo, lo, 1, 0, slot, dev_ap), remote(hi, hi, 1, 1, slot, dev_am))

        def s3():
            line = buf.at[core, pb]
            return (remote(line, line, 2, 0, slot, dev_bp), remote(line, line, 2, 1, slot, dev_bm))

        def s3_in():
            lo, hi = buf.at[core, b_dn], buf.at[core, b_up]
            return (remote(lo, lo, 2, 0, slot, dev_bp), remote(hi, hi, 2, 1, slot, dev_bm))

        def s4():
            lo, hi = buf.at[core, b_dn, pl.ds(0, side // 2)], buf.at[core, b_up, pl.ds(side // 2, side // 2)]
            return (remote(lo, lo, 3, 0, slot, dev_bp), remote(hi, hi, 3, 1, slot, dev_bm))

        def s4_in():
            far = lax.rem(pb + 2, side)
            lo, hi = buf.at[core, far, pl.ds(0, side // 2)], buf.at[core, far, pl.ds(side // 2, side // 2)]
            return (remote(lo, lo, 3, 0, slot, dev_bp), remote(hi, hi, 3, 1, slot, dev_bm))

        def hand(line, row, way):
            ref = buf.at[core, line]
            return remote(ref, ref, row, way, slot, sibling)

        def hand_in(line, row, way):
            ref = buf.at[1 - core, line]
            return remote(ref, ref, row, way, slot, sibling)

        def s3_all():
            return s3() + (hand(pb, 4, 0),)

        def s4_all():
            return s4() + (hand(b_dn, 4, 1), hand(b_up, 5, 0))

        def s5():
            return (hand(lax.rem(pb + 2, side), 5, 1),)

        def s5_in():
            return (hand_in(pa, 4, 0), hand_in(a_dn, 4, 1), hand_in(a_up, 5, 0), hand_in(lax.rem(pa + 2, side), 5, 1))

        outs = (s1, s2, s3_all, s4_all, s5)
        ins = (s1_in, s2_in, s3_in, s4_in, s5_in)

        def keep():
            return pltpu.make_async_copy(own, mine, own_sem.at[slot])

        if stage == 0:
            wait_own()
            keep().start()
        else:
            for d in outs[stage - 1]():
                d.wait_send()
            for d in ins[stage - 1]():
                d.wait_recv()
            if stage == 2:
                keep().wait()
        if stage < 5:
            for d in outs[stage]():
                d.start()

    def run_stage(stage, p):
        slot = lax.rem(p, SLOTS)

        @pl.when(p == 0)
        def _():
            stage_op(stage, wl_g, gath_g, wl_g.shape[0], SLOTS,
                     lambda: pltpu.make_async_copy(wl_g, wl_g, load_sem.at[n_piece]).wait())

        @pl.when(jnp.logical_and(p >= 0, p < first_d))
        def _():
            own = wl.at[p]
            stage_op(stage, own, gath.at[p], rows, slot,
                     lambda: pltpu.make_async_copy(own, own, load_sem.at[p]).wait())

        @pl.when(jnp.logical_and(p >= first_d, p < n_piece))
        def _():
            own = wl_d.at[p - first_d]
            stage_op(stage, own, gath_d.at[p - first_d], rows_d, slot,
                     lambda: pltpu.make_async_copy(own, own, load_sem.at[p]).wait())

    def tick(t):
        for stage in range(5):
            run_stage(stage, t - stage * LAG)
        run_stage(5, t - READY)

    def fetch(buf, dst, sem):
        cps = [pltpu.make_async_copy(buf.at[0], dst.at[:, :, 0], sem)]
        for y in range(side):
            cps.append(pltpu.make_async_copy(buf.at[1, :, y], dst.at[y, :, 1], sem))
        for cp in cps:
            cp.start()

    def fetch_piece(p):
        slot = lax.rem(p, 2)
        fetch(gath.at[p], wbuf.at[slot], wsem.at[slot])

    def wait_piece(p):
        slot = lax.rem(p, 2)
        pltpu.make_async_copy(wbuf.at[slot], wbuf.at[slot], wsem.at[slot]).wait()
        return slot

    def down_sem(slot, y):
        return wsem.at[2 + slot * side + y]

    def fetch_down(i):
        slot = lax.rem(i, 2)
        for y in range(side):
            pltpu.make_async_copy(gath_d.at[i, 0, y], wbuf_d.at[slot, y, :, 0], down_sem(slot, y)).start()
            pltpu.make_async_copy(gath_d.at[i, 1, :, y], wbuf_d.at[slot, y, :, 1], down_sem(slot, y)).start()

    def row_loop(body, block=rb):
        def step(i, carry):
            body(pl.ds(pl.multiple_of(i * block, block), block))
            return carry

        lax.fori_loop(0, seq // block, step, 0)

    def norm_rows(src, dst, gain_row):
        nb = min(64, seq)

        def body(rs):
            xx = src[rs, :].astype(F32)
            scale = lax.rsqrt(jnp.mean(xx * xx, axis=-1, keepdims=True) + NORM_EPS)
            dst[rs, :] = ((xx * scale) * gains[pl.ds(gain_row, 1), :]).astype(BF16)

        row_loop(body, nb)

    def weight(slot):
        return wbuf[slot].reshape(dim, width)

    lane = lax.broadcasted_iota(jnp.int32, (rb, 128), 1)
    low_half = lax.rem(lane, cfg["head"]) < cfg["head"] // 2

    def rope(block, rs):
        up = block.astype(BF16).astype(F32)
        swapped = jnp.where(low_half, pltpu.roll(up, 128 - cfg["head"] // 2, 1), pltpu.roll(up, cfg["head"] // 2, 1))
        return up * cosv[rs, :] + swapped * sinv[rs, :]

    n_kv = kv_dim // cfg["head"]
    head = cfg["head"]
    col_v = (0, n_kv * 128)
    col_k = (2 * n_kv * 128, 2 * n_kv * 128 + seq)

    def pre(t, carry):
        tick(t)
        return carry

    lax.fori_loop(0, LAG + 1, pre, 0)
    pltpu.make_async_copy(cos_hbm, cost, misc_sem.at[1]).wait()
    pltpu.make_async_copy(sin_hbm, sint, misc_sem.at[2]).wait()
    for k in range(seq // tb):
        cc, ss = cost[:, k * tb:(k + 1) * tb], sint[:, k * tb:(k + 1) * tb]
        cosv[k * tb:(k + 1) * tb, :] = jnp.transpose(jnp.concatenate([cc] * 4, axis=0))
        sinv[k * tb:(k + 1) * tb, :] = jnp.transpose(jnp.concatenate([-ss, ss] * 2, axis=0))
    lax.fori_loop(LAG + 1, READY + 1, pre, 0)
    fetch_piece(0)
    pltpu.sync_copy(gath_g, gvm)
    pltpu.make_async_copy(x_hbm, xv, misc_sem.at[0]).wait()
    lane8 = lax.broadcasted_iota(jnp.int32, (8, 128), 1)
    for y in range(side):
        for x in range(side):
            for which in range(2):
                even = gvm[0, y, x, 8 * which:8 * which + 8, :]
                odd = gvm[1, x, y, 8 * which:8 * which + 8, :]
                c = (y * side + x) * 128
                gains[8 * which:8 * which + 8, c:c + 128] = jnp.where(lane8 < 64, even, pltpu.roll(odd, 64, 1))
    norm_rows(xv, hbuf, 0)

    slot = wait_piece(0)

    def kv_block(rs):
        acc = jnp.dot(hbuf[rs, :], weight(slot), preferred_element_type=F32)
        first = lane < head
        for c in range(kv_dim // 128):
            kr = rope(acc[:, c * 128:(c + 1) * 128], rs)
            kt = jnp.transpose(kr).astype(BF16)
            kt_out[c * 128:(c + 1) * 128, rs] = kt
            zero = jnp.zeros((head, rs.size), BF16)
            for g in range(2):
                kk = kt[g * head:(g + 1) * head]
                r0 = (2 * c + g) * 128
                rbuf[r0:r0 + head, pl.ds(col_k[0] + rs.start, rs.size)] = kk
                rbuf[r0 + head:r0 + 128, pl.ds(col_k[0] + rs.start, rs.size)] = zero
                rbuf[r0:r0 + head, pl.ds(col_k[1] + rs.start, rs.size)] = zero
                rbuf[r0 + head:r0 + 128, pl.ds(col_k[1] + rs.start, rs.size)] = kk
            vv = acc[:, kv_dim + c * 128:kv_dim + (c + 1) * 128]
            vt = jnp.transpose(vv).astype(BF16)
            vt_out[c * 128:(c + 1) * 128, rs] = vt
            turned = pltpu.roll(vv, head, 1)
            g0, g1 = 2 * c, 2 * c + 1
            rbuf[rs, col_v[0] + g0 * 128:col_v[0] + g0 * 128 + 128] = jnp.where(first, vv, 0.0).astype(BF16)
            rbuf[rs, col_v[1] + g0 * 128:col_v[1] + g0 * 128 + 128] = jnp.where(first, 0.0, turned).astype(BF16)
            rbuf[rs, col_v[0] + g1 * 128:col_v[0] + g1 * 128 + 128] = jnp.where(first, turned, 0.0).astype(BF16)
            rbuf[rs, col_v[1] + g1 * 128:col_v[1] + g1 * 128 + 128] = jnp.where(first, 0.0, vv).astype(BF16)

    row_loop(kv_block)

    def q_step(c, carry):
        tick(READY + 1 + c)
        fetch_piece(1 + c)
        slot = wait_piece(1 + c)

        def q_block(rs):
            acc = jnp.dot(hbuf[rs, :], weight(slot), preferred_element_type=F32)
            for k in range(width // 128):
                dst = pl.ds(pl.multiple_of(c * width + k * 128, 128), 128)
                qbuf[rs, dst] = rope(acc[:, k * 128:(k + 1) * 128], rs).astype(BF16)

        row_loop(q_block)
        return carry

    lax.fori_loop(0, n_q, q_step, 0)
    t_now = READY + 1 + n_q

    n_pair = cfg["q_dim"] // 128
    pairs_per_kv = n_pair // n_kv
    qb = seq // len(ATTN_TICKS)
    scale = math.log2(math.e) * head ** -0.5
    causal = lax.broadcasted_iota(jnp.int32, (qb, qb), 0) >= lax.broadcasted_iota(jnp.int32, (qb, qb), 1)
    for i, n_t in enumerate(ATTN_TICKS):
        past = i * qb
        per = n_pair // n_t

        def one_pair(pi, i=i, past=past):
            g = pi // pairs_per_kv
            cs = pl.ds(pl.multiple_of(pi * 128, 128), 128)
            qp = qbuf[i * qb:(i + 1) * qb, cs]
            krow = pl.ds(pl.multiple_of(g * 128, 128), 128)
            total = None
            for hf in range(2):
                s_d = jnp.dot(qp, rbuf[krow, col_k[hf] + past:col_k[hf] + past + qb], preferred_element_type=F32)
                s_d = jnp.where(causal, s_d, -jnp.inf)
                m = jnp.max(s_d, axis=-1, keepdims=True)
                if past:
                    s_p = jnp.dot(qp, rbuf[krow, col_k[hf]:col_k[hf] + past], preferred_element_type=F32)
                    m = jnp.maximum(m, jnp.max(s_p, axis=-1, keepdims=True))
                e_d = jnp.exp2((s_d - m) * scale)
                den = jnp.sum(e_d, axis=-1, keepdims=True)
                if past:
                    e_p = jnp.exp2((s_p - m) * scale)
                    den = den + jnp.sum(e_p, axis=-1, keepdims=True)
                inv = 1.0 / den
                vcol = pl.ds(pl.multiple_of(col_v[hf] + g * 128, 128), 128)
                o = jnp.dot((e_d * inv).astype(BF16), rbuf[past:past + qb, vcol], preferred_element_type=F32)
                if past:
                    o = o + jnp.dot((e_p * inv).astype(BF16), rbuf[0:past, vcol], preferred_element_type=F32)
                total = o if total is None else total + o
            hbuf[i * qb:(i + 1) * qb, cs] = total.astype(BF16)

        def att_step(k, carry, one_pair=one_pair, per=per, base=t_now):
            tick(base + k)

            def inner(j, c2):
                one_pair(k * per + j)
                return c2

            lax.fori_loop(0, per, inner, 0)
            return carry

        lax.fori_loop(0, n_t, att_step, 0)
        t_now += n_t
        if i == 0:
            fetch_piece(first_o)

    def o_step(c, carry):
        tick(t_now + c)
        fetch_piece(first_o + 1 + c)
        slot = wait_piece(first_o + c)

        def o_block(rs):
            acc = jnp.dot(hbuf[rs, :], weight(slot), preferred_element_type=F32)
            cs = pl.ds(pl.multiple_of(c * width, width), width)
            xv[rs, cs] = (xv[rs, cs].astype(F32) + acc.astype(BF16).astype(F32)).astype(BF16)

        row_loop(o_block)
        return carry

    lax.fori_loop(0, n_o, o_step, 0)
    t_now += n_o
    norm_rows(xv, qbuf, 8)

    ticks_by = [min(j, FFN_PAIRED) // 2 + (j < FFN_PAIRED) + max(0, j - FFN_PAIRED + 1) + (j >= FFN_PAIRED) * (FFN_PAIRED % 2)
                for j in range(n_ffn)]
    early = [t_now - 1 + ticks_by[j] - READY >= first_f + j + 1 and j + 1 < n_ffn for j in range(n_ffn)]
    n_early = sum(early)
    assert all(early[:n_early]) and all(t_now - 1 + ticks_by[j] - READY >= first_f + j for j in range(n_ffn))

    def f_step(j, carry):
        @pl.when(jnp.logical_and(lax.rem(j, 2) == 0, j < FFN_PAIRED))
        def _():
            tick(t_now + j // 2)

        @pl.when(j >= FFN_PAIRED)
        def _():
            tick(t_now + (FFN_PAIRED + 1) // 2 + j - FFN_PAIRED)

        @pl.when(j > n_early)
        def _():
            fetch_piece(first_f + j)

        @pl.when(j < n_early)
        def _():
            fetch_piece(first_f + j + 1)

        slot = wait_piece(first_f + j)

        def f_block(rs):
            acc = jnp.dot(qbuf[rs, :], weight(slot), preferred_element_type=F32)
            gate = acc[:, :half_w].astype(BF16).astype(F32)
            up = acc[:, half_w:].astype(BF16).astype(F32)
            cs = pl.ds(pl.multiple_of(j * half_w, half_w), half_w)
            rbuf[rs, cs] = (jax.nn.silu(gate) * up).astype(BF16)

        row_loop(f_block)
        return carry

    lax.fori_loop(0, n_ffn, f_step, 0)
    t_now += ticks_by[-1]

    quarter = ffn // side

    def d_step(i, carry):
        tick(t_now + i)
        fetch_down(i)
        slot = lax.rem(i, 2)
        cs = pl.ds(pl.multiple_of(i * width_d, width_d), width_d)

        def add_rows(rs, acc):
            xv[rs, cs] = (xv[rs, cs].astype(F32) + acc.astype(BF16).astype(F32)).astype(BF16)

        acc = None
        for y in range(side):
            pltpu.make_async_copy(wbuf_d.at[slot, y], wbuf_d.at[slot, y], down_sem(slot, y)).wait()
            part = jnp.dot(rbuf[0:rb, y * quarter:(y + 1) * quarter], wbuf_d[slot, y].reshape(quarter, width_d),
                           preferred_element_type=F32)
            acc = part if acc is None else acc + part
        add_rows(pl.ds(0, rb), acc)

        def d_rows(k, c2):
            rs = pl.ds(pl.multiple_of(k * rb, rb), rb)
            add_rows(rs, jnp.dot(rbuf[rs, :], wbuf_d[slot].reshape(ffn, width_d), preferred_element_type=F32))
            return c2

        lax.fori_loop(1, seq // rb, d_rows, 0)
        return carry

    lax.fori_loop(0, n_down - 1, d_step, 0)

    def last_ticks(i, carry):
        tick(t_now + n_down - 1 + i)
        return carry

    lax.fori_loop(0, max(1, n_piece + READY - t_now - n_down + 1), last_ticks, 0)
    assert t_now + n_down >= n_piece + READY


def last_kernel(xv, rbuf, kt, vt, gath_d, out_hbm, kt_hbm, vt_hbm, wlast, tail, wsem, sems):
    seq, dim = xv.shape
    side = wlast.shape[0]
    width_d = tail.shape[1]
    done = dim - width_d
    last = gath_d.shape[0] - 1
    rb = min(ROW_BLOCK, seq)
    for y in range(side):
        pltpu.make_async_copy(gath_d.at[last, 0, y], wlast.at[y, :, 0], wsem.at[y]).start()
        pltpu.make_async_copy(gath_d.at[last, 1, :, y], wlast.at[y, :, 1], wsem.at[y]).start()
    copies = [pltpu.make_async_copy(xv.at[:, pl.ds(0, done)], out_hbm.at[:, pl.ds(0, done)], sems.at[0]),
              pltpu.make_async_copy(kt, kt_hbm, sems.at[1]), pltpu.make_async_copy(vt, vt_hbm, sems.at[2])]
    for cp in copies:
        cp.start()

    def rows_out(i):
        rs = pl.ds(pl.multiple_of(i * rb, rb), rb)
        return pltpu.make_async_copy(tail.at[rs], out_hbm.at[rs, pl.ds(done, width_d)], sems.at[3 + i])

    def finish_rows(i, acc):
        rs = pl.ds(pl.multiple_of(i * rb, rb), rb)
        tail[rs, :] = (xv[rs, done:].astype(F32) + acc.astype(BF16).astype(F32)).astype(BF16)
        rows_out(i).start()

    quarter = rbuf.shape[1] // side
    acc = None
    for y in range(side):
        pltpu.make_async_copy(wlast.at[y], wlast.at[y], wsem.at[y]).wait()
        part = jnp.dot(rbuf[0:rb, y * quarter:(y + 1) * quarter], wlast[y].reshape(quarter, width_d),
                       preferred_element_type=F32)
        acc = part if acc is None else acc + part
    finish_rows(0, acc)

    def block(i, carry):
        rs = pl.ds(pl.multiple_of(i * rb, rb), rb)
        finish_rows(i, jnp.dot(rbuf[rs, :], wlast[...].reshape(rbuf.shape[1], width_d), preferred_element_type=F32))
        return carry

    lax.fori_loop(1, seq // rb, block, 0)
    for cp in copies:
        cp.wait()
    for i in range(seq // rb):
        rows_out(i).wait()


def last_piece(xv, rbuf, kt, vt, gath_d):
    _, _, side, _, rows_d, width_d = gath_d.shape
    seq, dim = xv.shape
    vm, hbm = pl.BlockSpec(memory_space=pltpu.VMEM), pl.BlockSpec(memory_space=pl.ANY)
    return pl.pallas_call(
        last_kernel, in_specs=[vm] * 4 + [hbm], out_specs=[hbm] * 3,
        out_shape=[jax.ShapeDtypeStruct(t.shape, t.dtype) for t in (xv, kt, vt)],
        scratch_shapes=[
            pltpu.VMEM((side, side, 2, rows_d, width_d), BF16),
            pltpu.VMEM((seq, width_d), BF16),
            pltpu.SemaphoreType.DMA((side,)),
            pltpu.SemaphoreType.DMA((3 + seq // min(ROW_BLOCK, seq),)),
        ],
        compiler_params=pltpu.CompilerParams(vmem_limit_bytes=16 << 20),
    )(xv, rbuf, kt, vt, gath_d)


def solution(mesh, width=1024, width_d=256):
    n_dev = mesh.shape["fsdp"]
    side = math.isqrt(n_dev // 2)
    tok_spec = P(("dp", "fsdp"), None, None)
    cache_spec = P(("dp", "fsdp"), None, None, None)
    row_spec = P("fsdp", None)
    gain_spec = P("fsdp")
    table_spec = P(None, None)

    def local_layer(hidden, g_attn, w_query, w_key, w_value, w_out, g_mlp, w_gate, w_up, w_down, cos_tab, sin_tab):
        _, seq, dim = hidden.shape
        rows, q_dim = w_query.shape
        kv_dim = w_key.shape[1]
        ffn = w_gate.shape[1]
        rows_d = w_down.shape[0]
        head = 2 * cos_tab.shape[1]
        cfg = dict(side=side, seq=seq, dim=dim, ffn=ffn, width=width, width_d=width_d, kv_dim=kv_dim, q_dim=q_dim,
                   rows=rows, rows_d=rows_d, head=head)
        assert 2 * kv_dim == width and rows == 64 and rows * n_dev == dim
        wide = [jnp.pad(g.astype(F32), (0, 128 - rows))[None, :] for g in (g_attn, g_mlp)]
        gain_tile = jnp.concatenate([jnp.broadcast_to(g, (8, 128)) for g in wide])
        n_wide = (2 * kv_dim + q_dim + dim + 2 * ffn) // width
        n_down = dim // width_d
        n_piece = n_wide + n_down
        hbm = pl.BlockSpec(memory_space=pl.ANY)
        res = pl.pallas_call(
            functools.partial(layer_kernel, cfg),
            out_shape=(
                pltpu.VMEM((seq, dim), BF16),
                pltpu.VMEM((max(seq, 2 * kv_dim), ffn), BF16),
                pltpu.VMEM((kv_dim, seq), BF16),
                pltpu.VMEM((kv_dim, seq), BF16),
                jax.ShapeDtypeStruct((n_wide, 2, side, side, rows, width), BF16),
                jax.ShapeDtypeStruct((n_down, 2, side, side, rows_d, width_d), BF16),
                jax.ShapeDtypeStruct((2, side, side, 16, 128), F32)),
            in_specs=[hbm] * 11,
            out_specs=[pl.BlockSpec(memory_space=pltpu.VMEM)] * 4 + [hbm] * 3,
            scratch_shapes=[
                pltpu.VMEM((seq, max(dim, q_dim)), BF16),
                pltpu.VMEM((seq, max(dim, q_dim)), BF16),
                pltpu.VMEM((2, side, side, 2, rows, width), BF16),
                pltpu.VMEM((2, side, side, 2, rows_d, width_d), BF16),
                pltpu.VMEM((n_wide, rows, width), BF16),
                pltpu.VMEM((n_down, rows_d, width_d), BF16),
                pltpu.VMEM((16, 128), F32),
                pltpu.VMEM((2, side, side, 16, 128), F32),
                pltpu.VMEM((16, dim), F32),
                pltpu.VMEM((seq, 128), F32),
                pltpu.VMEM((seq, 128), F32),
                pltpu.VMEM((head // 2, seq), F32),
                pltpu.VMEM((head // 2, seq), F32),
                pltpu.SemaphoreType.DMA((6, 2, SLOTS + 1)),
                pltpu.SemaphoreType.DMA((6, 2, SLOTS + 1)),
                pltpu.SemaphoreType.DMA((SLOTS + 1,)),
                pltpu.SemaphoreType.DMA((n_piece + 1,)),
                pltpu.SemaphoreType.DMA((2 + 2 * side,)),
                pltpu.SemaphoreType.DMA((3,)),
            ],
            compiler_params=pltpu.CompilerParams(
                collective_id=0, has_side_effects=True, vmem_limit_bytes=VMEM_MAIN),
        )(hidden[0], gain_tile, w_query, w_key, w_value, w_out, w_gate, w_up, w_down, cos_tab.T, sin_tab.T)
        out, kt, vt = last_piece(*res[:4], res[5])

        def cache(t):
            return jnp.transpose(t.reshape(1, kv_dim // head, head, seq), (0, 3, 1, 2))

        return out[None], cache(kt), cache(vt)

    return jax.shard_map(local_layer, mesh=mesh, in_specs=(tok_spec, gain_spec, row_spec, row_spec, row_spec, row_spec, gain_spec, row_spec, row_spec, row_spec, table_spec, table_spec), out_specs=(tok_spec, cache_spec, cache_spec), check_vma=False)
```

```python
import functools
import math
import jax
import jax.numpy as jnp
from jax import lax
from jax.experimental import pallas as pl
from jax.experimental.pallas import tpu as pltpu
from jax.sharding import PartitionSpec as P

NORM_EPS = 1e-5
MESH = pl.DeviceIdType.MESH
LAG = 2
SLOTS = 2 * LAG + 4
READY = 4 * LAG + 1
ATTN_TICKS = (1, 1, 2, 2)
FFN_PAIRED = 13
ROW_BLOCK = 256
VMEM_MAIN = 38 << 20
BF16 = jnp.bfloat16
F32 = jnp.float32


def layer_kernel(cfg, x_hbm, gain_hbm, wq, wk, wv, wo, wg, wu, wd, cos_hbm, sin_hbm,
                 xv, rbuf, kt_out, vt_out, accv, gath, gath_d, gath_g,
                 hbuf, qbuf, wbuf, wbuf_d, wl, wl_d, wl_g, gvm, gains, cosv, sinv, cost, sint,
                 send_sem, recv_sem, own_sem, load_sem, wsem, misc_sem):
    side, seq, dim, ffn = cfg["side"], cfg["seq"], cfg["dim"], cfg["ffn"]
    width, half_w, width_d = cfg["width"], cfg["width"] // 2, cfg["width_d"]
    kv_dim = cfg["kv_dim"]
    n_q, n_o = cfg["q_dim"] // width, dim // width
    n_ffn, n_down = ffn // half_w, dim // width_d
    first_o = 1 + n_q
    first_f = first_o + n_o
    first_d = first_f + n_ffn
    n_piece = first_d + n_down
    rows, rows_d = cfg["rows"], cfg["rows_d"]
    rb = min(ROW_BLOCK, seq)
    tb = min(128, seq)

    me = lax.axis_index("fsdp")
    core = lax.rem(me, 2)
    px = lax.rem(me // 2, side)
    py = me // (2 * side)
    pa = px + core * (py - px)
    pb = py + core * (px - py)
    a_up, a_dn = lax.rem(pa + 1, side), lax.rem(pa + side - 1, side)
    b_up, b_dn = lax.rem(pb + 1, side), lax.rem(pb + side - 1, side)

    def device_at(a, b):
        y = b + core * (a - b)
        x = a + core * (b - a)
        return (y * side + x) * 2 + core

    dev_ap, dev_am = device_at(a_up, pb), device_at(a_dn, pb)
    dev_bp, dev_bm = device_at(pa, b_up), device_at(pa, b_dn)
    sibling = me + 1 - 2 * core

    def load(src, dst, sem):
        pltpu.make_async_copy(src, dst, sem).start()

    load(gain_hbm, wl_g, load_sem.at[n_piece])
    load(wk, wl.at[0, :, pl.ds(0, kv_dim)], load_sem.at[0])
    load(wv, wl.at[0, :, pl.ds(kv_dim, kv_dim)], load_sem.at[0])
    for c in range(n_q):
        load(wq.at[:, pl.ds(c * width, width)], wl.at[1 + c], load_sem.at[1 + c])
    load(x_hbm, xv, misc_sem.at[0])
    load(cos_hbm, cost, misc_sem.at[1])
    load(sin_hbm, sint, misc_sem.at[2])
    for c in range(n_o):
        load(wo.at[:, pl.ds(c * width, width)], wl.at[first_o + c], load_sem.at[first_o + c])

    def load_ffn(j, carry):
        col = pl.multiple_of(j * half_w, half_w)
        load(wg.at[:, pl.ds(col, half_w)], wl.at[first_f + j, :, pl.ds(0, half_w)], load_sem.at[first_f + j])
        load(wu.at[:, pl.ds(col, half_w)], wl.at[first_f + j, :, pl.ds(half_w, half_w)], load_sem.at[first_f + j])
        return carry

    lax.fori_loop(0, n_ffn, load_ffn, 0)

    def load_down(j, carry):
        col = pl.multiple_of(j * width_d, width_d)
        load(wd.at[:, pl.ds(col, width_d)], wl_d.at[j], load_sem.at[first_d + j])
        return carry

    lax.fori_loop(0, n_down, load_down, 0)

    dp = lax.axis_index("dp")
    barrier = pltpu.get_barrier_semaphore()
    for peer in (dev_ap, dev_am, dev_bp, dev_bm, sibling):
        pl.semaphore_signal(barrier, inc=1, device_id=(dp, peer), device_id_type=MESH)
    pl.semaphore_wait(barrier, 5)

    def remote(src, dst, stage, way, slot, peer):
        return pltpu.make_async_remote_copy(
            src_ref=src, dst_ref=dst, send_sem=send_sem.at[stage, way, slot], recv_sem=recv_sem.at[stage, way, slot],
            device_id=(dp, peer), device_id_type=MESH)

    def stage_op(stage, own, buf, n_rows, slot, wait_own):
        h = n_rows // 2
        mine = buf.at[core, pb, pa]

        def s1():
            return (remote(own, mine, 0, 0, slot, dev_ap), remote(own, mine, 0, 1, slot, dev_am))

        def s1_in():
            lo, hi = buf.at[core, pb, a_dn], buf.at[core, pb, a_up]
            return (remote(lo, lo, 0, 0, slot, dev_ap), remote(hi, hi, 0, 1, slot, dev_am))

        def s2():
            lo, hi = buf.at[core, pb, a_dn, pl.ds(0, h)], buf.at[core, pb, a_up, pl.ds(h, h)]
            return (remote(lo, lo, 1, 0, slot, dev_ap), remote(hi, hi, 1, 1, slot, dev_am))

        def s2_in():
            far = lax.rem(pa + 2, side)
            lo, hi = buf.at[core, pb, far, pl.ds(0, h)], buf.at[core, pb, far, pl.ds(h, h)]
            return (remote(lo, lo, 1, 0, slot, dev_ap), remote(hi, hi, 1, 1, slot, dev_am))

        def s3():
            line = buf.at[core, pb]
            return (remote(line, line, 2, 0, slot, dev_bp), remote(line, line, 2, 1, slot, dev_bm))

        def s3_in():
            lo, hi = buf.at[core, b_dn], buf.at[core, b_up]
            return (remote(lo, lo, 2, 0, slot, dev_bp), remote(hi, hi, 2, 1, slot, dev_bm))

        def s4():
            lo, hi = buf.at[core, b_dn, pl.ds(0, side // 2)], buf.at[core, b_up, pl.ds(side // 2, side // 2)]
            return (remote(lo, lo, 3, 0, slot, dev_bp), remote(hi, hi, 3, 1, slot, dev_bm))

        def s4_in():
            far = lax.rem(pb + 2, side)
            lo, hi = buf.at[core, far, pl.ds(0, side // 2)], buf.at[core, far, pl.ds(side // 2, side // 2)]
            return (remote(lo, lo, 3, 0, slot, dev_bp), remote(hi, hi, 3, 1, slot, dev_bm))

        def hand(line, row, way):
            ref = buf.at[core, line]
            return remote(ref, ref, row, way, slot, sibling)

        def hand_in(line, row, way):
            ref = buf.at[1 - core, line]
            return remote(ref, ref, row, way, slot, sibling)

        def s3_all():
            return s3() + (hand(pb, 4, 0),)

        def s4_all():
            return s4() + (hand(b_dn, 4, 1), hand(b_up, 5, 0))

        def s5():
            return (hand(lax.rem(pb + 2, side), 5, 1),)

        def s5_in():
            return (hand_in(pa, 4, 0), hand_in(a_dn, 4, 1), hand_in(a_up, 5, 0), hand_in(lax.rem(pa + 2, side), 5, 1))

        outs = (s1, s2, s3_all, s4_all, s5)
        ins = (s1_in, s2_in, s3_in, s4_in, s5_in)

        def keep():
            return pltpu.make_async_copy(own, mine, own_sem.at[slot])

        if stage == 0:
            wait_own()
            keep().start()
        else:
            for d in outs[stage - 1]():
                d.wait_send()
            for d in ins[stage - 1]():
                d.wait_recv()
            if stage == 2:
                keep().wait()
        if stage < 5:
            for d in outs[stage]():
                d.start()

    def run_stage(stage, p):
        slot = lax.rem(p, SLOTS)

        @pl.when(p == 0)
        def _():
            stage_op(stage, wl_g, gath_g, wl_g.shape[0], SLOTS,
                     lambda: pltpu.make_async_copy(wl_g, wl_g, load_sem.at[n_piece]).wait())

        @pl.when(jnp.logical_and(p >= 0, p < first_d))
        def _():
            own = wl.at[p]
            stage_op(stage, own, gath.at[p], rows, slot,
                     lambda: pltpu.make_async_copy(own, own, load_sem.at[p]).wait())

        @pl.when(jnp.logical_and(p >= first_d, p < n_piece))
        def _():
            own = wl_d.at[p - first_d]
            stage_op(stage, own, gath_d.at[p - first_d], rows_d, slot,
                     lambda: pltpu.make_async_copy(own, own, load_sem.at[p]).wait())

    def tick(t):
        for stage in range(5):
            run_stage(stage, t - stage * LAG)
        run_stage(5, t - READY)

    def fetch(buf, dst, sem):
        cps = [pltpu.make_async_copy(buf.at[0], dst.at[:, :, 0], sem)]
        for y in range(side):
            cps.append(pltpu.make_async_copy(buf.at[1, :, y], dst.at[y, :, 1], sem))
        for cp in cps:
            cp.start()

    def fetch_piece(p):
        slot = lax.rem(p, 2)
        fetch(gath.at[p], wbuf.at[slot], wsem.at[slot])

    def wait_piece(p):
        slot = lax.rem(p, 2)
        pltpu.make_async_copy(wbuf.at[slot], wbuf.at[slot], wsem.at[slot]).wait()
        return slot

    half = ffn // 2

    def down_copy(i, c, which):
        slot = lax.rem(i, 2)
        return pltpu.make_async_copy(gath_d.at[i, c], wbuf_d.at[slot, c], wsem.at[2 + slot * 2 + which])

    def down_dot(i, c, rs):
        lhs = rbuf[rs, pl.ds(pl.multiple_of(c * half, 128), half)]
        return jnp.dot(lhs, wbuf_d[lax.rem(i, 2), c].reshape(half, width_d), preferred_element_type=F32)

    def row_loop(body, block=rb):
        def step(i, carry):
            body(pl.ds(pl.multiple_of(i * block, block), block))
            return carry

        lax.fori_loop(0, seq // block, step, 0)

    def norm_rows(src, dst, gain_row):
        nb = min(64, seq)

        def body(rs):
            xx = src[rs, :].astype(F32)
            scale = lax.rsqrt(jnp.mean(xx * xx, axis=-1, keepdims=True) + NORM_EPS)
            dst[rs, :] = ((xx * scale) * gains[pl.ds(gain_row, 1), :]).astype(BF16)

        row_loop(body, nb)

    def weight(slot):
        return wbuf[slot].reshape(dim, width)

    lane = lax.broadcasted_iota(jnp.int32, (rb, 128), 1)
    low_half = lax.rem(lane, cfg["head"]) < cfg["head"] // 2

    def rope(block, rs):
        up = block.astype(BF16).astype(F32)
        swapped = jnp.where(low_half, pltpu.roll(up, 128 - cfg["head"] // 2, 1), pltpu.roll(up, cfg["head"] // 2, 1))
        return up * cosv[rs, :] + swapped * sinv[rs, :]

    n_kv = kv_dim // cfg["head"]
    head = cfg["head"]
    col_v = (0, n_kv * 128)
    col_k = (2 * n_kv * 128, 2 * n_kv * 128 + seq)

    def pre(t, carry):
        tick(t)
        return carry

    lax.fori_loop(0, LAG + 1, pre, 0)
    pltpu.make_async_copy(cos_hbm, cost, misc_sem.at[1]).wait()
    pltpu.make_async_copy(sin_hbm, sint, misc_sem.at[2]).wait()
    for k in range(seq // tb):
        cc, ss = cost[:, k * tb:(k + 1) * tb], sint[:, k * tb:(k + 1) * tb]
        cosv[k * tb:(k + 1) * tb, :] = jnp.transpose(jnp.concatenate([cc] * 4, axis=0))
        sinv[k * tb:(k + 1) * tb, :] = jnp.transpose(jnp.concatenate([-ss, ss] * 2, axis=0))
    lax.fori_loop(LAG + 1, READY + 1, pre, 0)
    fetch_piece(0)
    pltpu.sync_copy(gath_g, gvm)
    pltpu.make_async_copy(x_hbm, xv, misc_sem.at[0]).wait()
    lane8 = lax.broadcasted_iota(jnp.int32, (8, 128), 1)
    for y in range(side):
        for x in range(side):
            for which in range(2):
                even = gvm[0, y, x, 8 * which:8 * which + 8, :]
                odd = gvm[1, x, y, 8 * which:8 * which + 8, :]
                c = (y * side + x) * 128
                gains[8 * which:8 * which + 8, c:c + 128] = jnp.where(lane8 < 64, even, pltpu.roll(odd, 64, 1))
    norm_rows(xv, hbuf, 0)

    slot = wait_piece(0)

    def kv_block(rs):
        acc = jnp.dot(hbuf[rs, :], weight(slot), preferred_element_type=F32)
        first = lane < head
        for c in range(kv_dim // 128):
            kr = rope(acc[:, c * 128:(c + 1) * 128], rs)
            kt = jnp.transpose(kr).astype(BF16)
            kt_out[c * 128:(c + 1) * 128, rs] = kt
            zero = jnp.zeros((head, rs.size), BF16)
            for g in range(2):
                kk = kt[g * head:(g + 1) * head]
                r0 = (2 * c + g) * 128
                rbuf[r0:r0 + head, pl.ds(col_k[0] + rs.start, rs.size)] = kk
                rbuf[r0 + head:r0 + 128, pl.ds(col_k[0] + rs.start, rs.size)] = zero
                rbuf[r0:r0 + head, pl.ds(col_k[1] + rs.start, rs.size)] = zero
                rbuf[r0 + head:r0 + 128, pl.ds(col_k[1] + rs.start, rs.size)] = kk
            vv = acc[:, kv_dim + c * 128:kv_dim + (c + 1) * 128]
            vt = jnp.transpose(vv).astype(BF16)
            vt_out[c * 128:(c + 1) * 128, rs] = vt
            turned = pltpu.roll(vv, head, 1)
            g0, g1 = 2 * c, 2 * c + 1
            rbuf[rs, col_v[0] + g0 * 128:col_v[0] + g0 * 128 + 128] = jnp.where(first, vv, 0.0).astype(BF16)
            rbuf[rs, col_v[1] + g0 * 128:col_v[1] + g0 * 128 + 128] = jnp.where(first, 0.0, turned).astype(BF16)
            rbuf[rs, col_v[0] + g1 * 128:col_v[0] + g1 * 128 + 128] = jnp.where(first, turned, 0.0).astype(BF16)
            rbuf[rs, col_v[1] + g1 * 128:col_v[1] + g1 * 128 + 128] = jnp.where(first, 0.0, vv).astype(BF16)

    row_loop(kv_block)

    def q_step(c, carry):
        tick(READY + 1 + c)
        fetch_piece(1 + c)
        slot = wait_piece(1 + c)

        def q_block(rs):
            acc = jnp.dot(hbuf[rs, :], weight(slot), preferred_element_type=F32)
            for k in range(width // 128):
                dst = pl.ds(pl.multiple_of(c * width + k * 128, 128), 128)
                qbuf[rs, dst] = rope(acc[:, k * 128:(k + 1) * 128], rs).astype(BF16)

        row_loop(q_block)
        return carry

    lax.fori_loop(0, n_q, q_step, 0)
    t_now = READY + 1 + n_q

    n_pair = cfg["q_dim"] // 128
    pairs_per_kv = n_pair // n_kv
    qb = seq // len(ATTN_TICKS)
    scale = math.log2(math.e) * head ** -0.5
    causal = lax.broadcasted_iota(jnp.int32, (qb, qb), 0) >= lax.broadcasted_iota(jnp.int32, (qb, qb), 1)
    for i, n_t in enumerate(ATTN_TICKS):
        past = i * qb
        per = n_pair // n_t

        def one_pair(pi, i=i, past=past):
            g = pi // pairs_per_kv
            cs = pl.ds(pl.multiple_of(pi * 128, 128), 128)
            qp = qbuf[i * qb:(i + 1) * qb, cs]
            krow = pl.ds(pl.multiple_of(g * 128, 128), 128)
            total = None
            for hf in range(2):
                s_d = jnp.dot(qp, rbuf[krow, col_k[hf] + past:col_k[hf] + past + qb], preferred_element_type=F32)
                s_d = jnp.where(causal, s_d, -jnp.inf)
                m = jnp.max(s_d, axis=-1, keepdims=True)
                if past:
                    s_p = jnp.dot(qp, rbuf[krow, col_k[hf]:col_k[hf] + past], preferred_element_type=F32)
                    m = jnp.maximum(m, jnp.max(s_p, axis=-1, keepdims=True))
                e_d = jnp.exp2((s_d - m) * scale)
                den = jnp.sum(e_d, axis=-1, keepdims=True)
                if past:
                    e_p = jnp.exp2((s_p - m) * scale)
                    den = den + jnp.sum(e_p, axis=-1, keepdims=True)
                inv = 1.0 / den
                vcol = pl.ds(pl.multiple_of(col_v[hf] + g * 128, 128), 128)
                o = jnp.dot((e_d * inv).astype(BF16), rbuf[past:past + qb, vcol], preferred_element_type=F32)
                if past:
                    o = o + jnp.dot((e_p * inv).astype(BF16), rbuf[0:past, vcol], preferred_element_type=F32)
                total = o if total is None else total + o
            hbuf[i * qb:(i + 1) * qb, cs] = total.astype(BF16)

        def att_step(k, carry, one_pair=one_pair, per=per, base=t_now):
            tick(base + k)

            def inner(j, c2):
                one_pair(k * per + j)
                return c2

            lax.fori_loop(0, per, inner, 0)
            return carry

        lax.fori_loop(0, n_t, att_step, 0)
        t_now += n_t
        if i == 0:
            fetch_piece(first_o)

    def o_step(c, carry):
        tick(t_now + c)
        fetch_piece(first_o + 1 + c)
        slot = wait_piece(first_o + c)

        def o_block(rs):
            acc = jnp.dot(hbuf[rs, :], weight(slot), preferred_element_type=F32)
            cs = pl.ds(pl.multiple_of(c * width, width), width)
            xv[rs, cs] = (xv[rs, cs].astype(F32) + acc.astype(BF16).astype(F32)).astype(BF16)

        row_loop(o_block)
        return carry

    lax.fori_loop(0, n_o, o_step, 0)
    t_now += n_o
    norm_rows(xv, qbuf, 8)

    ticks_by = [min(j, FFN_PAIRED) // 2 + (j < FFN_PAIRED) + max(0, j - FFN_PAIRED + 1) + (j >= FFN_PAIRED) * (FFN_PAIRED % 2)
                for j in range(n_ffn)]
    early = [t_now - 1 + ticks_by[j] - READY >= first_f + j + 1 and j + 1 < n_ffn for j in range(n_ffn)]
    n_early = sum(early)
    assert all(early[:n_early]) and all(t_now - 1 + ticks_by[j] - READY >= first_f + j for j in range(n_ffn))

    def f_step(j, carry):
        @pl.when(jnp.logical_and(lax.rem(j, 2) == 0, j < FFN_PAIRED))
        def _():
            tick(t_now + j // 2)

        @pl.when(j >= FFN_PAIRED)
        def _():
            tick(t_now + (FFN_PAIRED + 1) // 2 + j - FFN_PAIRED)

        @pl.when(j > n_early)
        def _():
            fetch_piece(first_f + j)

        @pl.when(j < n_early)
        def _():
            fetch_piece(first_f + j + 1)

        slot = wait_piece(first_f + j)

        def f_block(rs):
            acc = jnp.dot(qbuf[rs, :], weight(slot), preferred_element_type=F32)
            gate = acc[:, :half_w].astype(BF16).astype(F32)
            up = acc[:, half_w:].astype(BF16).astype(F32)
            act = (jax.nn.silu(gate) * up).astype(BF16)
            chip_t = lax.rem(j, side) * side + j // side
            rbuf[rs, pl.ds(pl.multiple_of(j * rows_d, 128), rows_d)] = act[:, :rows_d]
            rbuf[rs, pl.ds(pl.multiple_of(half + chip_t * rows_d, 128), rows_d)] = act[:, rows_d:]

        row_loop(f_block)
        return carry

    lax.fori_loop(0, n_ffn, f_step, 0)
    t_now += ticks_by[-1]

    def own_half(i):
        down_copy(i, core, 0).wait()

        def rows_own(rs):
            accv[rs, :] = down_dot(i, core, rs)

        row_loop(rows_own)

    down_copy(0, core, 0).start()

    def d_step(i, carry):
        tick(t_now + i)
        down_copy(i, 1 - core, 1).start()
        down_copy(i + 1, core, 0).start()
        own_half(i)
        down_copy(i, 1 - core, 1).wait()
        cs = pl.ds(pl.multiple_of(i * width_d, width_d), width_d)

        def rows_rest(rs):
            acc = accv[rs, :] + down_dot(i, 1 - core, rs)
            xv[rs, cs] = (xv[rs, cs].astype(F32) + acc.astype(BF16).astype(F32)).astype(BF16)

        row_loop(rows_rest)
        return carry

    lax.fori_loop(0, n_down - 1, d_step, 0)
    own_half(n_down - 1)

    def last_ticks(i, carry):
        tick(t_now + n_down - 1 + i)
        return carry

    lax.fori_loop(0, max(1, n_piece + READY - t_now - n_down + 1), last_ticks, 0)
    assert t_now + n_down >= n_piece + READY and t_now - 1 - 4 * LAG >= first_d and half_w == 2 * rows_d


def last_kernel(xv, rbuf, kt, vt, accv, gath_d, out_hbm, kt_hbm, vt_hbm, wlast, tail, wsem, sems):
    seq, dim = xv.shape
    side, _, rows_d, width_d = wlast.shape
    done = dim - width_d
    last = gath_d.shape[0] - 1
    rb = min(ROW_BLOCK, seq)
    part_k = side * rows_d
    other = 1 - lax.rem(lax.axis_index("fsdp"), 2)
    base = other * (rbuf.shape[1] // 2)
    parts = [pltpu.make_async_copy(gath_d.at[last, other, b], wlast.at[b], wsem.at[b]) for b in range(side)]
    for cp in parts:
        cp.start()
    copies = [pltpu.make_async_copy(xv.at[:, pl.ds(0, done)], out_hbm.at[:, pl.ds(0, done)], sems.at[0]),
              pltpu.make_async_copy(kt, kt_hbm, sems.at[1]), pltpu.make_async_copy(vt, vt_hbm, sems.at[2])]

    def rows_out(i):
        rs = pl.ds(pl.multiple_of(i * rb, rb), rb)
        return pltpu.make_async_copy(tail.at[rs], out_hbm.at[rs, pl.ds(done, width_d)], sems.at[3 + i])

    def finish_rows(i, acc):
        rs = pl.ds(pl.multiple_of(i * rb, rb), rb)
        acc = accv[rs, :] + acc
        tail[rs, :] = (xv[rs, done:].astype(F32) + acc.astype(BF16).astype(F32)).astype(BF16)
        rows_out(i).start()

    acc = None
    for b in range(side):
        parts[b].wait()
        lhs = rbuf[0:rb, pl.ds(pl.multiple_of(base + b * part_k, 128), part_k)]
        part = jnp.dot(lhs, wlast[b].reshape(part_k, width_d), preferred_element_type=F32)
        acc = part if acc is None else acc + part
    for cp in copies:
        cp.start()
    finish_rows(0, acc)

    def block(i, carry):
        lhs = rbuf[pl.ds(pl.multiple_of(i * rb, rb), rb), pl.ds(pl.multiple_of(base, 128), side * part_k)]
        finish_rows(i, jnp.dot(lhs, wlast[...].reshape(side * part_k, width_d), preferred_element_type=F32))
        return carry

    lax.fori_loop(1, seq // rb, block, 0)
    for cp in copies:
        cp.wait()
    for i in range(seq // rb):
        rows_out(i).wait()


def last_piece(xv, rbuf, kt, vt, accv, gath_d):
    _, _, side, _, rows_d, width_d = gath_d.shape
    seq, dim = xv.shape
    vm, hbm = pl.BlockSpec(memory_space=pltpu.VMEM), pl.BlockSpec(memory_space=pl.ANY)
    return pl.pallas_call(
        last_kernel, in_specs=[vm] * 5 + [hbm], out_specs=[hbm] * 3,
        out_shape=[jax.ShapeDtypeStruct(t.shape, t.dtype) for t in (xv, kt, vt)],
        scratch_shapes=[
            pltpu.VMEM((side, side, rows_d, width_d), BF16),
            pltpu.VMEM((seq, width_d), BF16),
            pltpu.SemaphoreType.DMA((side,)),
            pltpu.SemaphoreType.DMA((3 + seq // min(ROW_BLOCK, seq),)),
        ],
        compiler_params=pltpu.CompilerParams(vmem_limit_bytes=16 << 20),
    )(xv, rbuf, kt, vt, accv, gath_d)


def solution(mesh, width=1024, width_d=256):
    n_dev = mesh.shape["fsdp"]
    side = math.isqrt(n_dev // 2)
    tok_spec = P(("dp", "fsdp"), None, None)
    cache_spec = P(("dp", "fsdp"), None, None, None)
    row_spec = P("fsdp", None)
    gain_spec = P("fsdp")
    table_spec = P(None, None)

    def local_layer(hidden, g_attn, w_query, w_key, w_value, w_out, g_mlp, w_gate, w_up, w_down, cos_tab, sin_tab):
        _, seq, dim = hidden.shape
        rows, q_dim = w_query.shape
        kv_dim = w_key.shape[1]
        ffn = w_gate.shape[1]
        rows_d = w_down.shape[0]
        head = 2 * cos_tab.shape[1]
        cfg = dict(side=side, seq=seq, dim=dim, ffn=ffn, width=width, width_d=width_d, kv_dim=kv_dim, q_dim=q_dim,
                   rows=rows, rows_d=rows_d, head=head)
        assert 2 * kv_dim == width and rows == 64 and rows * n_dev == dim
        both = jnp.stack([g_attn, g_mlp]).astype(F32)
        gain_tile = jnp.broadcast_to(jnp.pad(both, ((0, 0), (0, 128 - rows)))[:, None, :], (2, 8, 128)).reshape(16, 128)
        n_wide = (2 * kv_dim + q_dim + dim + 2 * ffn) // width
        n_down = dim // width_d
        n_piece = n_wide + n_down
        hbm = pl.BlockSpec(memory_space=pl.ANY)
        res = pl.pallas_call(
            functools.partial(layer_kernel, cfg),
            out_shape=(
                pltpu.VMEM((seq, dim), BF16),
                pltpu.VMEM((max(seq, 2 * kv_dim), ffn), BF16),
                pltpu.VMEM((kv_dim, seq), BF16),
                pltpu.VMEM((kv_dim, seq), BF16),
                pltpu.VMEM((seq, width_d), F32),
                jax.ShapeDtypeStruct((n_wide, 2, side, side, rows, width), BF16),
                jax.ShapeDtypeStruct((n_down, 2, side, side, rows_d, width_d), BF16),
                jax.ShapeDtypeStruct((2, side, side, 16, 128), F32)),
            in_specs=[hbm] * 11,
            out_specs=[pl.BlockSpec(memory_space=pltpu.VMEM)] * 5 + [hbm] * 3,
            scratch_shapes=[
                pltpu.VMEM((seq, max(dim, q_dim)), BF16),
                pltpu.VMEM((seq, max(dim, q_dim)), BF16),
                pltpu.VMEM((2, side, side, 2, rows, width), BF16),
                pltpu.VMEM((2, 2, side, side, rows_d, width_d), BF16),
                pltpu.VMEM((n_wide, rows, width), BF16),
                pltpu.VMEM((n_down, rows_d, width_d), BF16),
                pltpu.VMEM((16, 128), F32),
                pltpu.VMEM((2, side, side, 16, 128), F32),
                pltpu.VMEM((16, dim), F32),
                pltpu.VMEM((seq, 128), F32),
                pltpu.VMEM((seq, 128), F32),
                pltpu.VMEM((head // 2, seq), F32),
                pltpu.VMEM((head // 2, seq), F32),
                pltpu.SemaphoreType.DMA((6, 2, SLOTS + 1)),
                pltpu.SemaphoreType.DMA((6, 2, SLOTS + 1)),
                pltpu.SemaphoreType.DMA((SLOTS + 1,)),
                pltpu.SemaphoreType.DMA((n_piece + 1,)),
                pltpu.SemaphoreType.DMA((6,)),
                pltpu.SemaphoreType.DMA((3,)),
            ],
            compiler_params=pltpu.CompilerParams(
                collective_id=0, has_side_effects=True, vmem_limit_bytes=VMEM_MAIN),
        )(hidden[0], gain_tile, w_query, w_key, w_value, w_out, w_gate, w_up, w_down, cos_tab.T, sin_tab.T)
        out, kt, vt = last_piece(*res[:5], res[6])

        def cache(t):
            return jnp.transpose(t.reshape(1, kv_dim // head, head, seq), (0, 3, 1, 2))

        return out[None], cache(kt), cache(vt)

    return jax.shard_map(local_layer, mesh=mesh, in_specs=(tok_spec, gain_spec, row_spec, row_spec, row_spec, row_spec, gain_spec, row_spec, row_spec, row_spec, table_spec, table_spec), out_specs=(tok_spec, cache_spec, cache_spec), check_vma=False)
```
